8 devices in a mesh: dp: 1 (over z), tp: 8 (over y, x, core).
Axes of the slice: x: 2, y: 2, z: 1, core: 2. Of those that a mesh axis runs over, the one named last changes fastest.
Arguments:
- x_in: bfloat16 [512, 7168], P('dp')
- pos_ids: int32 [512], P('dp')
- ckv_cache: bfloat16 [2, 512, 256, 512], P(None, 'dp')
- kpe_cache: bfloat16 [2, 512, 256, 64], P(None, 'dp')
- attn_gain: bfloat16 [2, 7168], replicated
- w_dq: bfloat16 [2, 7168, 1536], replicated
- q_gain: bfloat16 [2, 1536], replicated
- w_dkv: bfloat16 [2, 7168, 576], replicated
- kv_gain: bfloat16 [2, 512], replicated
- w_uq: bfloat16 [2, 1536, 64, 192], P(None, None, 'tp')
- w_uk: bfloat16 [2, 512, 64, 128], P(None, None, 'tp')
- w_uv: bfloat16 [2, 512, 64, 128], P(None, None, 'tp')
- w_o: bfloat16 [2, 64, 128, 7168], P(None, 'tp')
- mlp_gain: bfloat16 [2, 7168], replicated
- w_gate: bfloat16 [2, 7168, 9216], P(None, None, 'tp')
- w_up: bfloat16 [2, 7168, 9216], P(None, None, 'tp')
- w_down: bfloat16 [2, 9216, 7168], P(None, 'tp')
Outputs:
- output 1: bfloat16 [512, 7168], P('dp')
- output 2: bfloat16 [2, 512, 512], P(None, 'dp')
- output 3: bfloat16 [2, 512, 64], P(None, 'dp')
All inputs are finite; a program needn't handle non-finite values.
Results may differ from the reference program's by a relative error of at most 0.02.
Values are sent between devices in bfloat16 or wider.
A program may use at most 2 GiB of HBM per device.

```python
import math
import jax
import jax.numpy as jnp
from jax import lax

SEQ_COUNT = 512
CACHE_LEN = 256
MODEL_DIM = 7168
FFN_DIM = 9216
NUM_HEADS = 64
Q_LORA = 1536
KV_LORA = 512
ROPE_DIM = 64
NOPE_DIM = 128
VALUE_DIM = 128
LAYER_COUNT = 2
ROPE_BASE = 10000

NORM_EPS = 1e-6
SCORE_SCALE = (NOPE_DIM + ROPE_DIM) ** -0.5


def rms_norm(values, norm_gain):
    values = values.astype(jnp.float32)
    inv_rms = lax.rsqrt(jnp.mean(values * values, axis=-1, keepdims=True) + NORM_EPS)
    return (values * inv_rms * norm_gain.astype(jnp.float32)).astype(jnp.bfloat16)


def rotary(values, positions):
    half_dim = ROPE_DIM // 2
    inv_freq = jnp.exp(jnp.arange(half_dim, dtype=jnp.float32) * (-2.0 * math.log(ROPE_BASE) / ROPE_DIM))
    angles = positions.astype(jnp.float32)[..., None] * inv_freq
    cos_part = jnp.cos(angles)
    sin_part = jnp.sin(angles)
    lo_half = values[..., :half_dim]
    hi_half = values[..., half_dim:]
    return jnp.concatenate([lo_half * cos_part - hi_half * sin_part, hi_half * cos_part + lo_half * sin_part], axis=-1)


def draw_normal(key, shape, std_dev):
    return (jax.random.normal(key, shape, jnp.float32) * std_dev).astype(jnp.bfloat16)


def draw_gain(key, width):
    return (1.0 + 0.25 * jax.random.normal(key, (LAYER_COUNT, width), jnp.float32)).astype(jnp.bfloat16)


def setup_inputs(seed: int = 0, part: int = 0) -> dict:
    shared_keys = jax.random.split(jax.random.key(seed), 16)
    local_keys = jax.random.split(jax.random.fold_in(jax.random.key(seed + 1), part), 6)
    qk_dim = NOPE_DIM + ROPE_DIM
    low_pos = CACHE_LEN // 2
    pos_ids = jax.random.randint(local_keys[1], (SEQ_COUNT,), low_pos, CACHE_LEN, jnp.int32)
    pos_ids = pos_ids.at[0].set(CACHE_LEN - 1).at[1].set(low_pos)
    seq_mean = jax.random.normal(local_keys[2], (LAYER_COUNT, SEQ_COUNT, 1, KV_LORA), jnp.float32)
    cache_noise = jax.random.normal(local_keys[3], (LAYER_COUNT, SEQ_COUNT, CACHE_LEN, KV_LORA), jnp.float32)
    return {
        'x_in': draw_normal(local_keys[0], (SEQ_COUNT, MODEL_DIM), 1.0),
        'pos_ids': pos_ids,
        'ckv_cache': (0.8 * seq_mean + 0.6 * cache_noise).astype(jnp.bfloat16),
        'kpe_cache': draw_normal(local_keys[4], (LAYER_COUNT, SEQ_COUNT, CACHE_LEN, ROPE_DIM), 1.0),
        'attn_gain': draw_gain(shared_keys[0], MODEL_DIM),
        'w_dq': draw_normal(shared_keys[1], (LAYER_COUNT, MODEL_DIM, Q_LORA), MODEL_DIM ** -0.5),
        'q_gain': draw_gain(shared_keys[2], Q_LORA),
        'w_dkv': draw_normal(shared_keys[3], (LAYER_COUNT, MODEL_DIM, KV_LORA + ROPE_DIM), MODEL_DIM ** -0.5),
        'kv_gain': draw_gain(shared_keys[4], KV_LORA),
        'w_uq': draw_normal(shared_keys[5], (LAYER_COUNT, Q_LORA, NUM_HEADS, qk_dim), Q_LORA ** -0.5),
        'w_uk': draw_normal(shared_keys[6], (LAYER_COUNT, KV_LORA, NUM_HEADS, NOPE_DIM), 3.0 * NOPE_DIM ** -0.5),
        'w_uv': draw_normal(shared_keys[7], (LAYER_COUNT, KV_LORA, NUM_HEADS, VALUE_DIM), KV_LORA ** -0.5),
        'w_o': draw_normal(shared_keys[8], (LAYER_COUNT, NUM_HEADS, VALUE_DIM, MODEL_DIM), (NUM_HEADS * VALUE_DIM) ** -0.5),
        'mlp_gain': draw_gain(shared_keys[9], MODEL_DIM),
        'w_gate': draw_normal(shared_keys[10], (LAYER_COUNT, MODEL_DIM, FFN_DIM), MODEL_DIM ** -0.5),
        'w_up': draw_normal(shared_keys[11], (LAYER_COUNT, MODEL_DIM, FFN_DIM), MODEL_DIM ** -0.5),
        'w_down': draw_normal(shared_keys[12], (LAYER_COUNT, FFN_DIM, MODEL_DIM), FFN_DIM ** -0.5),
    }


def attend_one(seq_item):
    q_lat, q_rope, ckv_seq, kpe_seq, position = seq_item
    scores = jnp.dot(q_lat, ckv_seq.T, preferred_element_type=jnp.float32)
    scores = (scores + jnp.dot(q_rope, kpe_seq.T, preferred_element_type=jnp.float32)) * SCORE_SCALE
    visible = jnp.arange(CACHE_LEN)[None, :] <= position
    scores = jnp.where(visible, scores, -jnp.inf)
    attn_prob = jax.nn.softmax(scores, axis=-1).astype(jnp.bfloat16)
    return jnp.dot(attn_prob, ckv_seq, preferred_element_type=jnp.float32).astype(jnp.bfloat16)


def one_layer(hidden, pos_ids, layer_in):
    (ckv_old, kpe_old, attn_gain, w_dq, q_gain, w_dkv, kv_gain, w_uq, w_uk, w_uv, w_o, mlp_gain, w_gate, w_up, w_down) = layer_in
    normed = rms_norm(hidden, attn_gain)
    c_q = rms_norm(jnp.dot(normed, w_dq, preferred_element_type=jnp.float32), q_gain)
    q_full = jnp.einsum('bc,chd->bhd', c_q.astype(jnp.float32), w_uq.astype(jnp.float32))
    q_nope = q_full[..., :NOPE_DIM].astype(jnp.bfloat16)
    q_rope = rotary(q_full[..., NOPE_DIM:], pos_ids[:, None]).astype(jnp.bfloat16)
    q_lat = jnp.einsum('bhn,chn->bhc', q_nope.astype(jnp.float32), w_uk.astype(jnp.float32)).astype(jnp.bfloat16)
    kv_lat = jnp.dot(normed, w_dkv, preferred_element_type=jnp.float32)
    ckv_new = rms_norm(kv_lat[:, :KV_LORA], kv_gain)
    kpe_new = rotary(kv_lat[:, KV_LORA:], pos_ids).astype(jnp.bfloat16)
    at_pos = (jnp.arange(CACHE_LEN)[None, :] == pos_ids[:, None])[:, :, None]
    ckv_all = jnp.where(at_pos, ckv_new[:, None, :], ckv_old)
    kpe_all = jnp.where(at_pos, kpe_new[:, None, :], kpe_old)
    context = lax.map(attend_one, (q_lat, q_rope, ckv_all, kpe_all, pos_ids))
    head_out = jnp.einsum('bhc,chv->bhv', context.astype(jnp.float32), w_uv.astype(jnp.float32)).astype(jnp.bfloat16)
    attn_sum = jnp.einsum('bhv,hvd->bd', head_out.astype(jnp.float32), w_o.astype(jnp.float32))
    mid_state = (hidden.astype(jnp.float32) + attn_sum).astype(jnp.bfloat16)
    mlp_in = rms_norm(mid_state, mlp_gain)
    gate_pre = jnp.dot(mlp_in, w_gate, preferred_element_type=jnp.float32)
    up_pre = jnp.dot(mlp_in, w_up, preferred_element_type=jnp.float32)
    act_out = (jax.nn.silu(gate_pre) * up_pre).astype(jnp.bfloat16)
    mlp_sum = jnp.dot(act_out, w_down, preferred_element_type=jnp.float32)
    layer_out = (mid_state.astype(jnp.float32) + mlp_sum).astype(jnp.bfloat16)
    return layer_out, (ckv_new, kpe_new)


def reference(x_in, pos_ids, ckv_cache, kpe_cache, attn_gain, w_dq, q_gain, w_dkv, kv_gain, w_uq, w_uk, w_uv, w_o, mlp_gain, w_gate, w_up, w_down):
    def layer_step(hidden, layer_in):
        return one_layer(hidden, pos_ids, layer_in)
    stacked = (ckv_cache, kpe_cache, attn_gain, w_dq, q_gain, w_dkv, kv_gain, w_uq, w_uk, w_uv, w_o, mlp_gain, w_gate, w_up, w_down)
    x_out, (ckv_rows, kpe_rows) = lax.scan(layer_step, x_in, stacked)
    return x_out, ckv_rows, kpe_rows
```

```python
import functools
import math
import jax
import jax.numpy as jnp
from jax import lax
from jax.experimental import pallas as pl
from jax.experimental.pallas import tpu as pltpu
from jax.sharding import PartitionSpec as P

NORM_EPS = 1e-6
ROPE_BASE = 10000.0
BF = jnp.bfloat16
F32 = jnp.float32
NT = (((1,), (1,)), ((), ()))
MESH = pl.DeviceIdType.MESH

SUB = 8
CHUNKS = 4
WIDE = 1024

ORDER_LAST = (
    'O00', 'O01', 'O02', 'A000', 'O03', 'A001', 'A002', 'A003', 'A100', 'A200', 'A101', 'B000', 'A102', 'A201',
    'A103', 'A202', 'B001', 'B100', 'B200', 'M10', 'B101', 'B002', 'A203', 'A010', 'B201', 'M11', 'B102', 'B003',
    'A011', 'A110', 'B202', 'M12', 'B103', 'A210', 'A012', 'B203', 'M13', 'B010', 'A111', 'A112', 'A013', 'A211',
    'B110', 'A212', 'B210', 'A113', 'B011', 'B012', 'B111', 'A213', 'B211', 'B112', 'B013', 'B212', 'B113', 'B213',
)
ORDER_MID = (
    'O00', 'O01', 'O02', 'A000', 'O03', 'A001', 'A002', 'A003', 'A100', 'A200', 'A101', 'B000', 'A102', 'A201',
    'A103', 'A202', 'B001', 'B100', 'B200', 'M10', 'B101', 'B002', 'A203', 'A010', 'B201', 'M11', 'B102', 'B003',
    'A011', 'A110', 'B202', 'M12', 'B103', 'A210', 'A012', 'B203', 'M13', 'A111', 'A112', 'A013', 'A211', 'A212',
    'A113', 'A213',
)


def rms_norm(values, norm_gain):
    values = values.astype(F32)
    inv_rms = lax.rsqrt(jnp.mean(values * values, axis=-1, keepdims=True) + NORM_EPS)
    return (values * inv_rms * norm_gain.astype(F32)).astype(BF)


def rotate(values, cos_part, sin_part):
    half_dim = values.shape[-1] // 2
    lo_half = values[..., :half_dim]
    hi_half = values[..., half_dim:]
    return jnp.concatenate([lo_half * cos_part - hi_half * sin_part, hi_half * cos_part + lo_half * sin_part], axis=-1)


def attn_body(sb, nslot, steps, layer, scale, pos_ref, q_ref, r_ref, c_hbm, k_hbm, cn_ref, kn_ref, o_ref, cbuf, kbuf, s_ref, f_ref, csem, ksem):
    heads = q_ref.shape[1]
    step = pl.program_id(0)
    base = step * sb
    nsub = sb // SUB
    total = steps * nsub

    def copies(t, slot):
        return (pltpu.make_async_copy(c_hbm.at[layer, pl.ds(t * SUB, SUB)], cbuf.at[slot], csem.at[slot]),
                pltpu.make_async_copy(k_hbm.at[layer, pl.ds(t * SUB, SUB)], kbuf.at[slot], ksem.at[slot]))

    @pl.when(step == 0)
    def _():
        for t in range(nslot):
            for c in copies(t, t):
                c.start()

    par = lax.rem(step, nslot // nsub) * nsub
    for i in range(sb):
        f_ref[i * heads:(i + 1) * heads, :] = jnp.full((heads, 128), pos_ref[base + i], jnp.int32)
    for j in range(nsub):
        slot = par + j
        for c in copies(step * nsub + j, slot):
            c.wait()
        for i in range(j * SUB, (j + 1) * SUB):
            s = lax.dot_general(q_ref[i], cbuf[slot, i - j * SUB], NT, preferred_element_type=F32)
            s_ref[i * heads:(i + 1) * heads, :] = s + jnp.dot(r_ref[i], kbuf[slot, i - j * SUB], preferred_element_type=F32)
    n = sb * heads
    col = lax.broadcasted_iota(jnp.int32, (n, s_ref.shape[1]), 1)
    pv = f_ref[:, 0:1]
    cn = cn_ref[...].astype(F32)[:, None, :]
    fresh = jnp.sum(q_ref[...].astype(F32) * cn, axis=-1, keepdims=True)
    fresh = fresh + jnp.sum(r_ref[...].astype(F32) * kn_ref[...].astype(F32)[:, None, :], axis=-1, keepdims=True)
    hit = col == pv
    s = jnp.where(hit, fresh.reshape(n, 1), s_ref[...]) * scale
    s = jnp.where(col <= pv, s, -jnp.inf)
    e = jnp.exp(s - jnp.max(s, axis=-1, keepdims=True))
    w = (e / jnp.sum(e, axis=-1, keepdims=True)).astype(BF).astype(F32)
    new_prob = jnp.sum(jnp.where(hit, w, 0.0), axis=-1, keepdims=True)
    new_part = new_prob.reshape(sb, heads, 1) * cn
    s_ref[...] = jnp.where(hit, 0.0, w)
    for j in range(nsub):
        slot = par + j
        for i in range(j * SUB, (j + 1) * SUB):
            ctx = jnp.dot(s_ref[i * heads:(i + 1) * heads, :].astype(BF), cbuf[slot, i - j * SUB], preferred_element_type=F32)
            o_ref[i] = (ctx + new_part[i]).astype(BF)
        nxt = step * nsub + j + nslot

        @pl.when(nxt < total)
        def _():
            for c in copies(nxt, slot):
                c.start()


def latent_attention(q_lat, q_rope, ckv, kpe_t, c_new, k_new, pos, layer, scale, sb=32, nslot=8):
    n, heads, lat = q_lat.shape
    rope = q_rope.shape[-1]
    keys = ckv.shape[2]

    def im3(b, p):
        return (b, 0, 0)

    spec = pltpu.PrefetchScalarGridSpec(
        num_scalar_prefetch=1, grid=(n // sb,),
        in_specs=[pl.BlockSpec((sb, heads, lat), im3), pl.BlockSpec((sb, heads, rope), im3),
                  pl.BlockSpec(memory_space=pl.ANY), pl.BlockSpec(memory_space=pl.ANY),
                  pl.BlockSpec((sb, lat), lambda b, p: (b, 0)), pl.BlockSpec((sb, rope), lambda b, p: (b, 0))],
        out_specs=pl.BlockSpec((sb, heads, lat), im3),
        scratch_shapes=[pltpu.VMEM((nslot, SUB, keys, lat), BF), pltpu.VMEM((nslot, SUB, rope, keys), BF),
                        pltpu.VMEM((sb * heads, keys), F32), pltpu.VMEM((sb * heads, 128), jnp.int32),
                        pltpu.SemaphoreType.DMA((nslot,)), pltpu.SemaphoreType.DMA((nslot,))])
    return pl.pallas_call(
        functools.partial(attn_body, sb, nslot, n // sb, layer, scale), grid_spec=spec, name='mla_attn',
        out_shape=jax.ShapeDtypeStruct((n, heads, lat), BF),
        compiler_params=pltpu.CompilerParams(dimension_semantics=('arbitrary',)),
        cost_estimate=pl.CostEstimate(flops=2 * n * heads * keys * (2 * lat + rope), bytes_accessed=n * keys * (lat + rope) * 2, transcendentals=n * heads * keys),
    )(pos, q_lat, q_rope, ckv, kpe_t, c_new, k_new)


def post_body(layer, last, *refs):
    if last:
        (ho_ref, x_hbm, gain_ref, wo_hbm, wg_hbm, wu_hbm, wd_hbm,
         out_hbm, wgu, wod, buf, r0, r1, r2, own, act, wsem, gsem, xsem, osem, ss, rs, ack) = refs
    else:
        (ho_ref, x_hbm, gain_ref, wo_hbm, wg_hbm, wu_hbm, wd_hbm,
         next_gain_ref, q_gain_ref, kv_gain_ref, cos_hbm, sin_hbm, wdq_hbm, wdkv_hbm,
         own_out, cq_out, ckv_out, kpe_out,
         wgu, wod, buf, r0, r1, r2, own, act, cos_v, sin_v, wsem, gsem, xsem, osem, ss, rs, ack) = refs
    depth = wo_hbm.shape[1]
    cols = wd_hbm.shape[1]
    width = wd_hbm.shape[2]
    rows = buf.shape[1]
    half, quart, eighth = rows // 2, rows // 4, rows // 8
    tiles = width // WIDE

    me = lax.axis_index('tp')
    c = lax.rem(me, 2)
    x = lax.rem(me // 2, 2)
    y = me // 4
    f = x * (1 - c) + y * c
    s = y * (1 - c) + x * c
    pair = y * 4 + x * 2 + (1 - c)
    n1 = (y * (1 - c) + (1 - y) * c) * 4 + ((1 - x) * (1 - c) + x * c) * 2 + c
    n2 = ((1 - y) * (1 - c) + y * c) * 4 + (x * (1 - c) + (1 - x) * c) * 2 + c
    half_own, half_oth = c * half, (1 - c) * half
    quart_own, quart_oth = half_own + f * quart, half_own + (1 - f) * quart
    eig_own, eig_oth = quart_own + s * eighth, quart_own + (1 - s) * eighth
    al = lambda v: pl.multiple_of(v, 16)

    barrier = pltpu.get_barrier_semaphore()
    for dev in (pair, n1, n2):
        pl.semaphore_signal(barrier, inc=1, device_id={'tp': dev}, device_id_type=MESH)

    wo_cp = [pltpu.make_async_copy(wo_hbm.at[layer, :, pl.ds(j * WIDE, WIDE)], wod.at[pl.ds(0, depth), pl.ds(j * WIDE, WIDE)], wsem.at[j]) for j in range(tiles)]
    for cp in wo_cp:
        cp.start()
    if last:
        x_cp = [pltpu.make_async_copy(x_hbm, own, xsem.at[0])]
    else:
        x_cp = [pltpu.make_async_copy(x_hbm.at[:, pl.ds(al(eig_own), eighth)], own, xsem.at[0]),
                pltpu.make_async_copy(cos_hbm.at[:, pl.ds(al(eig_own), eighth)], cos_v, xsem.at[1]),
                pltpu.make_async_copy(sin_hbm.at[:, pl.ds(al(eig_own), eighth)], sin_v, xsem.at[2])]
    for cp in x_cp:
        cp.start()
    gu_cp = []
    for j in range(cols // 128):
        gu_cp.append(pltpu.make_async_copy(wg_hbm.at[layer, :, pl.ds(j * 128, 128)], wgu.at[:, pl.ds(2 * j * 128, 128)], gsem.at[2 * j]))
        gu_cp.append(pltpu.make_async_copy(wu_hbm.at[layer, :, pl.ds(j * 128, 128)], wgu.at[:, pl.ds((2 * j + 1) * 128, 128)], gsem.at[2 * j + 1]))
    wd_cp = [pltpu.make_async_copy(wd_hbm.at[layer, :, pl.ds(j * WIDE, WIDE)], wod.at[:, pl.ds(j * WIDE, WIDE)], wsem.at[j]) for j in range(tiles)]
    if not last:
        dq = wdq_hbm.shape[2]
        dkv = wdkv_hbm.shape[1]
        lat = kv_gain_ref.shape[1]
        dq_cp = [pltpu.make_async_copy(wdq_hbm.at[layer + 1, :, pl.ds(j * 256, 256)], wgu.at[:, pl.ds(j * 256, 256)], gsem.at[j]) for j in range(dq // 256)]
        dkv_cp = [pltpu.make_async_copy(wdkv_hbm.at[layer + 1], wod.at[pl.ds(0, dkv)], wsem.at[0])]
    pl.semaphore_wait(barrier, 3)

    sent = {}

    def send(kind, ph, r, dev):
        k = 6 * ph + ('S0', 'S1', 'S2', 'G0', 'G1', 'G2').index(kind)
        if kind == 'S0':
            src, dst = buf.at[r, pl.ds(al(half_oth), half)], r0.at[r]
        elif kind == 'S1':
            src, dst = buf.at[r, pl.ds(al(quart_oth), quart)], r1.at[r]
        elif kind == 'S2':
            src, dst = buf.at[r, pl.ds(al(eig_oth), eighth)], r2.at[r]
        else:
            off, n = {'G0': (eig_own, eighth), 'G1': (quart_own, quart), 'G2': (half_own, half)}[kind]
            src = buf.at[r, pl.ds(al(off), n)]
            dst = src
        cp = pltpu.make_async_remote_copy(src_ref=src, dst_ref=dst, send_sem=ss.at[k, r], recv_sem=rs.at[k, r],
                                          device_id={'tp': dev}, device_id_type=MESH)
        cp.start()
        sent[kind, ph, r] = cp

    def landed(kind, ph, r, dev):
        sent[kind, ph, r].wait_recv()
        sent[kind, ph, r].wait_send()
        pl.semaphore_signal(ack.at[3 * ph + int(kind[1]), r], inc=1, device_id={'tp': dev}, device_id_type=MESH)

    def granted(kind, ph, r):
        pl.semaphore_wait(ack.at[3 * ph + int(kind[1]), r], 1)

    def add_rows(r, off, src, src_off, n):
        def tile(t, _):
            cs = pl.ds(pl.multiple_of(t * WIDE, WIDE), WIDE)
            rw = pl.ds(al(off), n)
            buf[r, rw, cs] = (buf[r, rw, cs].astype(F32) + src[r, pl.ds(al(src_off), n), cs].astype(F32)).astype(BF)
            return 0
        lax.fori_loop(0, tiles, tile, 0)

    def step_o(r):
        if r == 0:
            for cp in x_cp:
                cp.wait()

        def tile(t, _):
            if r == 0:
                pltpu.make_async_copy(wo_hbm.at[layer, :, pl.ds(0, WIDE)], wod.at[pl.ds(0, depth), pl.ds(0, WIDE)], wsem.at[t]).wait()
            cs = pl.ds(pl.multiple_of(t * WIDE, WIDE), WIDE)
            buf[r, :, cs] = jnp.dot(ho_ref[r], wod[0:depth, cs], preferred_element_type=F32).astype(BF)
            return 0
        lax.fori_loop(0, tiles, tile, 0)
        send('S0', 0, r, pair)
        if r == 0:
            for cp in gu_cp:
                cp.start()
        if r == CHUNKS - 1:
            for cp in wd_cp:
                cp.start()

    def step_m(r):
        if r == 0:
            for cp in gu_cp:
                cp.wait()

        def gate(j, _):
            cs = pl.ds(pl.multiple_of(j * 256, 256), 256)
            pre = jnp.dot(buf[r], wgu[:, cs], preferred_element_type=F32)
            act[:, pl.ds(pl.multiple_of(j * 128, 128), 128)] = (jax.nn.silu(pre[:, :128]) * pre[:, 128:]).astype(BF)
            return 0
        lax.fori_loop(0, cols // 128, gate, 0)
        if r == CHUNKS - 1 and not last:
            for cp in dq_cp:
                cp.start()
        if r == 0:
            for cp in wd_cp:
                cp.wait()
        for kind in ('G0', 'G1', 'G2'):
            sent[kind, 0, r].wait_send()

        def tile(t, _):
            cs = pl.ds(pl.multiple_of(t * WIDE, WIDE), WIDE)
            buf[r, :, cs] = jnp.dot(act[...], wod[:, cs], preferred_element_type=F32).astype(BF)
            return 0
        lax.fori_loop(0, tiles, tile, 0)
        send('S0', 1, r, pair)
        if r == CHUNKS - 1 and not last:
            for cp in dkv_cp:
                cp.start()

    def reduce_own(ph, r):
        def tile(t, acc):
            cs = pl.ds(pl.multiple_of(t * WIDE, WIDE), WIDE)
            v = own[r, :, cs].astype(F32) + (buf[r, pl.ds(al(eig_own), eighth), cs].astype(F32) + r2[r, :, cs].astype(F32))
            v = v.astype(BF)
            own[r, :, cs] = v
            if ph == 1 and last:
                buf[r, pl.ds(al(eig_own), eighth), cs] = v
            v = v.astype(F32)
            return acc + v * v
        acc = lax.fori_loop(0, tiles, tile, jnp.zeros((eighth, WIDE), F32))
        return lax.rsqrt(jnp.sum(acc, axis=-1, keepdims=True) * (1.0 / width) + NORM_EPS)

    def norm_own(r, inv, gain, put):
        def tile(t, _):
            cs = pl.ds(pl.multiple_of(t * WIDE, WIDE), WIDE)
            put(r, cs, (own[r, :, cs].astype(F32) * inv * gain[:, cs].astype(F32)).astype(BF))
            return 0
        lax.fori_loop(0, tiles, tile, 0)

    def put_buf(r, cs, v):
        buf[r, pl.ds(al(eig_own), eighth), cs] = v

    def put_r2(r, cs, v):
        r2[r, :, cs] = v

    for token in (ORDER_LAST if last else ORDER_MID):
        op, ph, r = token[:-2], int(token[-2]), int(token[-1])
        if op == 'O':
            step_o(r)
        elif op == 'M':
            step_m(r)
        elif op == 'A0':
            landed('S0', ph, r, pair)
            add_rows(r, quart_oth, r0, (1 - f) * quart, quart)
            add_rows(r, quart_own, r0, f * quart, quart)
            send('S1', ph, r, n1)
        elif op == 'A1':
            landed('S1', ph, r, n1)
            add_rows(r, eig_oth, r1, (1 - s) * eighth, eighth)
            add_rows(r, eig_own, r1, s * eighth, eighth)
            send('S2', ph, r, n2)
        elif op == 'A2':
            landed('S2', ph, r, n2)
            inv = reduce_own(ph, r)
            if ph == 0:
                norm_own(r, inv, gain_ref, put_buf)
            elif not last:
                norm_own(r, inv, next_gain_ref, put_r2)
            if ph == 0 or last:
                granted('S2', ph, r)
                send('G0', ph, r, n2)
        elif op == 'B0':
            sent['G0', ph, r].wait_recv()
            granted('S1', ph, r)
            send('G1', ph, r, n1)
        elif op == 'B1':
            sent['G1', ph, r].wait_recv()
            granted('S0', ph, r)
            send('G2', ph, r, pair)
        elif op == 'B2':
            sent['G2', ph, r].wait_recv()
            if ph == 1:
                cp = pltpu.make_async_copy(buf.at[r], out_hbm.at[r], osem.at[r])
                cp.start()
                sent['out', 1, r] = cp

    if last:
        for r in range(CHUNKS):
            for kind in ('G0', 'G1', 'G2'):
                sent[kind, 1, r].wait_send()
            sent['out', 1, r].wait()
        return

    own_cp = pltpu.make_async_copy(own, own_out, osem.at[0])
    own_cp.start()
    n = CHUNKS * eighth
    mine = pl.ds(al(eig_own), eighth)
    a = r2[...].reshape(n, width)
    for cp in dkv_cp:
        cp.wait()
    kv = lax.dot_general(a, wod[0:lat, :], NT, preferred_element_type=F32)
    inv = lax.rsqrt(jnp.mean(kv * kv, axis=-1, keepdims=True) + NORM_EPS)
    buf[:, mine, dq:dq + lat] = (kv * inv * kv_gain_ref[...].astype(F32)).astype(BF).reshape(CHUNKS, eighth, lat)
    kp = lax.dot_general(a, wod[lat:lat + 128, :], NT, preferred_element_type=F32)
    rope = dkv - lat
    lane = lax.broadcasted_iota(jnp.int32, (n, 128), 1)
    swap = jnp.where(lane < rope // 2, pltpu.roll(kp, 128 - rope // 2, 1), pltpu.roll(kp, rope // 2, 1))
    kp = jnp.where(lane < rope, kp * cos_v[...].reshape(n, 128) + swap * sin_v[...].reshape(n, 128), 0.0)
    buf[:, mine, dq + lat:dq + lat + 128] = kp.astype(BF).reshape(CHUNKS, eighth, 128)
    for cp in dq_cp:
        cp.wait()
    cq = [jnp.dot(a, wgu[:, j * 512:(j + 1) * 512], preferred_element_type=F32) for j in range(dq // 512)]
    inv = lax.rsqrt(sum(jnp.sum(v * v, axis=-1, keepdims=True) for v in cq) * (1.0 / dq) + NORM_EPS)
    for j, v in enumerate(cq):
        buf[:, mine, j * 512:(j + 1) * 512] = (v * inv * q_gain_ref[:, j * 512:(j + 1) * 512].astype(F32)).astype(BF).reshape(CHUNKS, eighth, 512)

    used = dq + lat + 128

    def gather(k, off, rows_n, dev):
        part = buf.at[:, pl.ds(al(off), rows_n), pl.ds(0, used)]
        cp = pltpu.make_async_remote_copy(src_ref=part, dst_ref=part, send_sem=ss.at[k, 0], recv_sem=rs.at[k, 0],
                                          device_id={'tp': dev}, device_id_type=MESH)
        cp.start()
        return cp

    for r in range(CHUNKS):
        granted('S2', 1, r)
    g0 = gather(9, eig_own, eighth, n2)
    g0.wait_recv()
    for r in range(CHUNKS):
        granted('S1', 1, r)
    g1 = gather(10, quart_own, quart, n1)
    g1.wait_recv()
    for r in range(CHUNKS):
        granted('S0', 1, r)
    g2 = gather(11, half_own, half, pair)
    g2.wait_recv()
    outs = [pltpu.make_async_copy(buf.at[:, :, pl.ds(0, dq)], cq_out, osem.at[1]),
            pltpu.make_async_copy(buf.at[:, :, pl.ds(dq, lat)], ckv_out, osem.at[2]),
            pltpu.make_async_copy(buf.at[:, :, pl.ds(dq + lat, 128)], kpe_out, osem.at[3])]
    for cp in outs:
        cp.start()
    for cp in (g0, g1, g2):
        cp.wait_send()
    own_cp.wait()
    for cp in outs:
        cp.wait()


def post_layer(layer, last, head_out, resid, mlp_gain, w_o, w_gate, w_up, w_down, more):
    n, width = head_out.shape[0], w_down.shape[2]
    rows = n // CHUNKS
    depth, cols = w_o.shape[1], w_down.shape[1]
    vm = pl.BlockSpec(memory_space=pltpu.VMEM)
    hb = pl.BlockSpec(memory_space=pl.ANY)
    args = [head_out.reshape(CHUNKS, rows, depth), resid, mlp_gain, w_o, w_gate, w_up, w_down]
    specs = [vm, hb, vm, hb, hb, hb, hb]
    scratch = [pltpu.VMEM((width, 2 * cols), BF), pltpu.VMEM((cols, width), BF), pltpu.VMEM((CHUNKS, rows, width), BF),
               pltpu.VMEM((CHUNKS, rows // 2, width), BF), pltpu.VMEM((CHUNKS, rows // 4, width), BF),
               pltpu.VMEM((CHUNKS, rows // 8, width), BF), pltpu.VMEM((CHUNKS, rows // 8, width), BF),
               pltpu.VMEM((rows, cols), BF)]
    if last:
        outs = jax.ShapeDtypeStruct((CHUNKS, rows, width), BF)
        out_specs = hb
    else:
        next_gain, q_gain, kv_gain, cos_t, sin_t, w_dq, w_dkv_t = more
        args += [next_gain, q_gain, kv_gain, cos_t, sin_t, w_dq, w_dkv_t]
        specs += [vm, vm, vm, hb, hb, hb, hb]
        scratch += [pltpu.VMEM((CHUNKS, rows // 8, 128), F32)] * 2
        outs = (jax.ShapeDtypeStruct((CHUNKS, rows // 8, width), BF), jax.ShapeDtypeStruct((CHUNKS, rows, w_dq.shape[2]), BF),
                jax.ShapeDtypeStruct((CHUNKS, rows, kv_gain.shape[1]), BF), jax.ShapeDtypeStruct((CHUNKS, rows, 128), BF))
        out_specs = (hb,) * 4
    scratch += [pltpu.SemaphoreType.DMA((width // WIDE,)), pltpu.SemaphoreType.DMA((2 * cols // 128,)),
                pltpu.SemaphoreType.DMA((3,)), pltpu.SemaphoreType.DMA((4,)),
                pltpu.SemaphoreType.DMA((12, CHUNKS)), pltpu.SemaphoreType.DMA((12, CHUNKS)),
                pltpu.SemaphoreType.REGULAR((6, CHUNKS))]
    return pl.pallas_call(
        functools.partial(post_body, layer, last), in_specs=specs, out_specs=out_specs, out_shape=outs, scratch_shapes=scratch,
        name='post_last' if last else 'post_mid',
        compiler_params=pltpu.CompilerParams(collective_id=1 if last else 0, has_side_effects=True, vmem_limit_bytes=67043328),
        cost_estimate=pl.CostEstimate(flops=2 * n * width * (depth + 3 * cols), bytes_accessed=2 * width * (depth + 3 * cols), transcendentals=n * cols),
    )(*args)


def solution(mesh):
    cache_spec = P(None, 'dp', None, None)
    head_spec = P(None, None, 'tp', None)
    weight_specs = (P(), P(), P(), P(), P(), head_spec, head_spec, head_spec, P(None, 'tp', None, None), P(), P(None, None, 'tp'), P(None, None, 'tp'), P(None, 'tp', None))
    in_specs = (P('dp', None), P('dp'), cache_spec, cache_spec) + weight_specs
    out_specs = (P('dp', None), P(None, 'dp', None), P(None, 'dp', None))

    def device_body(x_in, pos_ids, ckv_cache, kpe_cache, attn_gain, w_dq, q_gain, w_dkv, kv_gain, w_uq, w_uk, w_uv, w_o, mlp_gain, w_gate, w_up, w_down):
        n, width = x_in.shape
        rows = n // CHUNKS
        lat = w_uk.shape[1]
        nope = w_uk.shape[3]
        rope = kpe_cache.shape[3]
        half = rope // 2
        inv_freq = jnp.exp(jnp.arange(half, dtype=F32) * (-2.0 * math.log(ROPE_BASE) / rope))
        angles = pos_ids.astype(F32)[:, None] * inv_freq
        cos_p, sin_p = jnp.cos(angles), jnp.sin(angles)
        pad = jnp.zeros((n, 128 - rope), F32)
        cos_t = jnp.concatenate([cos_p, cos_p, pad], axis=1).reshape(CHUNKS, rows, 128)
        sin_t = jnp.concatenate([-sin_p, sin_p, pad], axis=1).reshape(CHUNKS, rows, 128)
        kpe_t = jnp.swapaxes(kpe_cache, 2, 3)
        w_dkv_t = jnp.swapaxes(w_dkv, 1, 2)
        w_o2 = w_o.reshape(w_o.shape[0], -1, width)
        scale = w_uq.shape[-1] ** -0.5

        def heads_of(layer, c_q, c_new, k_new):
            q_full = jnp.einsum('bc,chd->bhd', c_q, w_uq[layer], preferred_element_type=F32)
            q_nope = q_full[..., :nope].astype(BF)
            q_rope = rotate(q_full[..., nope:], cos_p[:, None], sin_p[:, None]).astype(BF)
            q_lat = jnp.einsum('bhn,chn->bhc', q_nope, w_uk[layer], preferred_element_type=F32).astype(BF)
            ctx = latent_attention(q_lat, q_rope, ckv_cache, kpe_t, c_new, k_new, pos_ids, layer, scale)
            return jnp.einsum('bhc,chv->bhv', ctx, w_uv[layer], preferred_element_type=F32).astype(BF).reshape(n, -1)

        normed = rms_norm(x_in, attn_gain[0])
        c_q = rms_norm(jnp.dot(normed, w_dq[0], preferred_element_type=F32), q_gain[0])
        kv = jnp.dot(normed, w_dkv[0], preferred_element_type=F32)
        c_new0 = rms_norm(kv[:, :lat], kv_gain[0])
        k_new0 = rotate(kv[:, lat:], cos_p, sin_p).astype(BF)
        head_out = heads_of(0, c_q, c_new0, k_new0)
        x_own, c_q, c_new1, k_new1 = post_layer(
            0, False, head_out, x_in.reshape(CHUNKS, rows, width), mlp_gain[0:1], w_o2, w_gate, w_up, w_down,
            (attn_gain[1:2], q_gain[1:2], kv_gain[1:2], cos_t, sin_t, w_dq, w_dkv_t))
        c_new1 = c_new1.reshape(n, lat)
        k_new1 = k_new1.reshape(n, 128)[:, :rope]
        head_out = heads_of(1, c_q.reshape(n, -1), c_new1, k_new1)
        x_out = post_layer(1, True, head_out, x_own, mlp_gain[1:2], w_o2, w_gate, w_up, w_down, None)
        return x_out.reshape(n, width), jnp.stack([c_new0, c_new1]), jnp.stack([k_new0, k_new1])

    return jax.shard_map(device_body, mesh=mesh, in_specs=in_specs, out_specs=out_specs, check_vma=False)
```

```python
import functools
import math
import jax
import jax.numpy as jnp
from jax import lax
from jax.experimental import pallas as pl
from jax.experimental.pallas import tpu as pltpu
from jax.sharding import PartitionSpec as P

NORM_EPS = 1e-6
ROPE_BASE = 10000.0
BF = jnp.bfloat16
F32 = jnp.float32
NT = (((1,), (1,)), ((), ()))
MESH = pl.DeviceIdType.MESH

SUB = 8
STEP = 32
SUBS = 5
SLOTS = 12
CHUNKS = 4
WIDE = 1024

ORDER_LAST = (
    'T', 'T', 'T', 'T', 'O00', 'T', 'A000', 'T', 'T', 'A100', 'T', 'O01', 'A200', 'T',
    'A001', 'T', 'B000', 'T', 'A101', 'T', 'O02', 'B100', 'A201', 'T', 'B200', 'A002', 'T', 'B001',
    'T', 'A102', 'T', 'O03', 'B101', 'A202', 'M', 'M', 'B201', 'A003', 'M', 'B002', 'M', 'M',
    'M', 'A103', 'M', 'A010', 'M', 'M', 'B102', 'A203', 'M', 'B202', 'M', 'A110', 'A011', 'B003',
    'M', 'M', 'M', 'A210', 'M', 'A111', 'A012', 'B010', 'B103', 'A211', 'B203', 'M', 'M', 'A112',
    'M', 'B011', 'M', 'M', 'B110', 'A212', 'A013', 'B111', 'B210', 'B012', 'B211', 'A113', 'B112', 'A213',
    'B212', 'B013', 'B113', 'B213',
)
ORDER_MID = (
    'T', 'T', 'T', 'T', 'O00', 'T', 'A000', 'T', 'T', 'A100', 'T', 'O01', 'A200', 'T',
    'A001', 'T', 'B000', 'T', 'A101', 'T', 'O02', 'B100', 'A201', 'T', 'B200', 'A002', 'T', 'B001',
    'T', 'A102', 'T', 'O03', 'B101', 'A202', 'M', 'M', 'B201', 'A003', 'M', 'B002', 'M', 'M',
    'M', 'A103', 'M', 'A010', 'M', 'M', 'B102', 'A203', 'M', 'B202', 'M', 'A110', 'A011', 'B003',
    'M', 'M', 'M', 'A210', 'M', 'A111', 'A012', 'B103', 'A211', 'B203', 'M', 'M', 'A112', 'M',
    'M', 'M', 'A212', 'A013', 'A113', 'A213',
)


def rms_norm(values, norm_gain):
    values = values.astype(F32)
    inv_rms = lax.rsqrt(jnp.mean(values * values, axis=-1, keepdims=True) + NORM_EPS)
    return (values * inv_rms * norm_gain.astype(F32)).astype(BF)


def rotate(values, cos_part, sin_part):
    half_dim = values.shape[-1] // 2
    lo_half = values[..., :half_dim]
    hi_half = values[..., half_dim:]
    return jnp.concatenate([lo_half * cos_part - hi_half * sin_part, hi_half * cos_part + lo_half * sin_part], axis=-1)


def layer_body(layer, last, scale, *refs):
    (pos_ref, cn_ref, kn_ref, uv_ref, q_hbm, qr_hbm, ckv_hbm, kpe_hbm, x_hbm, gain_ref, wo_hbm, wg_hbm, wu_hbm, wd_hbm), refs = refs[:14], refs[14:]
    if last:
        out_hbm, refs = refs[0], refs[1:]
    else:
        (next_gain_ref, q_gain_ref, kv_gain_ref, cos_hbm, sin_hbm, wdq_hbm, wdkv_hbm, own_out, cq_out, ckv_out, kpe_out), refs = refs[:11], refs[11:]
    (wgu, wod, buf, r0, r1, r2, own, act, sc, ctx, posv, wsem, gsem, xsem, osem, ss, rs, ack, credit, csem, ksem, qsem, rsem), refs = refs[:23], refs[23:]
    if not last:
        cos_v, sin_v = refs
    heads = 8
    keys = sc.shape[1]
    n_lat = q_hbm.shape[1]
    n_rope = kpe_hbm.shape[1] // (ckv_hbm.shape[1] // keys)
    steps = q_hbm.shape[0] // (STEP * heads)
    total = steps * (STEP // SUB)
    q_base = 3 * SUB * keys
    k_col = 4 * n_lat
    depth = wo_hbm.shape[1]
    cols = wd_hbm.shape[1]
    width = wd_hbm.shape[2]
    rows = buf.shape[1]
    half, quart, eighth = rows // 2, rows // 4, rows // 8
    tiles = width // WIDE

    me = lax.axis_index('tp')
    c = lax.rem(me, 2)
    x = lax.rem(me // 2, 2)
    y = me // 4
    f = x * (1 - c) + y * c
    s = y * (1 - c) + x * c
    pair = y * 4 + x * 2 + (1 - c)
    n1 = (y * (1 - c) + (1 - y) * c) * 4 + ((1 - x) * (1 - c) + x * c) * 2 + c
    n2 = ((1 - y) * (1 - c) + y * c) * 4 + (x * (1 - c) + (1 - x) * c) * 2 + c
    half_own, half_oth = c * half, (1 - c) * half
    quart_own, quart_oth = half_own + f * quart, half_own + (1 - f) * quart
    eig_own, eig_oth = quart_own + s * eighth, quart_own + (1 - s) * eighth
    al = lambda v: pl.multiple_of(v, 16)

    barrier = pltpu.get_barrier_semaphore()
    for dev in (pair, n1, n2):
        pl.semaphore_signal(barrier, inc=1, device_id={'tp': dev}, device_id_type=MESH)

    def slot_at(slot):
        return pl.multiple_of(lax.rem(slot, 3) * (SUB * keys), SUB * keys), pl.multiple_of(slot // 3 * n_lat, n_lat)

    def cache_copies(t):
        slot = lax.rem(t, SLOTS)
        row, col = slot_at(slot)
        return (pltpu.make_async_copy(ckv_hbm.at[layer, pl.ds(pl.multiple_of(t * (SUB * keys), SUB * keys), SUB * keys)],
                                      wgu.at[pl.ds(row, SUB * keys), pl.ds(col, n_lat)], csem.at[slot]),
                pltpu.make_async_copy(kpe_hbm.at[layer, pl.ds(pl.multiple_of(t * (SUB * n_rope), SUB * n_rope), SUB * n_rope)],
                                      wgu.at[pl.ds(pl.multiple_of(slot * (SUB * n_rope), SUB * n_rope), SUB * n_rope), pl.ds(k_col, keys)], ksem.at[slot]))

    def q_at(k):
        return pl.multiple_of(q_base + lax.rem(k, 4) * (STEP * heads), STEP * heads), pl.multiple_of(k // 4 * n_lat, n_lat)

    def q_copies(k):
        row, col = q_at(k)
        n = STEP * heads
        out = [pltpu.make_async_copy(q_hbm.at[pl.ds(pl.multiple_of(k * n, n), n)], wgu.at[pl.ds(row, n), pl.ds(col, n_lat)], qsem.at[k])]
        for i in range(2):
            out.append(pltpu.make_async_copy(qr_hbm.at[pl.ds(pl.multiple_of(k * n + i * 128, 128), 128)],
                                             wod.at[pl.ds(depth, 128), pl.ds(pl.multiple_of((2 * k + i) * 128, 128), 128)], rsem.at[2 * k + i]))
        return out

    def start_all(cps):
        for cp in cps:
            cp.start()

    def wait_all(cps):
        for cp in cps:
            cp.wait()

    start_all(q_copies(0))
    for t in range(STEP // SUB):
        start_all(cache_copies(t))
    for k in range(1, steps):
        start_all(q_copies(k))
    for t in range(STEP // SUB, SLOTS):
        start_all(cache_copies(t))

    wo_cp = [pltpu.make_async_copy(wo_hbm.at[layer, :, pl.ds(j * WIDE, WIDE)], wod.at[pl.ds(0, depth), pl.ds(j * WIDE, WIDE)], wsem.at[j]) for j in range(tiles)]
    for cp in wo_cp:
        cp.start()
    if last:
        x_cp = [pltpu.make_async_copy(x_hbm, own, xsem.at[0])]
    else:
        x_cp = [pltpu.make_async_copy(x_hbm.at[:, pl.ds(al(eig_own), eighth)], own, xsem.at[0]),
                pltpu.make_async_copy(cos_hbm.at[:, pl.ds(al(eig_own), eighth)], cos_v, xsem.at[1]),
                pltpu.make_async_copy(sin_hbm.at[:, pl.ds(al(eig_own), eighth)], sin_v, xsem.at[2])]
    for cp in x_cp:
        cp.start()
    gu_cp = []
    for j in range(cols // 128):
        gu_cp.append(pltpu.make_async_copy(wg_hbm.at[layer, :, pl.ds(j * 128, 128)], wgu.at[:, pl.ds(2 * j * 128, 128)], gsem.at[2 * j]))
        gu_cp.append(pltpu.make_async_copy(wu_hbm.at[layer, :, pl.ds(j * 128, 128)], wgu.at[:, pl.ds((2 * j + 1) * 128, 128)], gsem.at[2 * j + 1]))
    wd_cp = [pltpu.make_async_copy(wd_hbm.at[layer, :, pl.ds(j * WIDE, WIDE)], wod.at[:, pl.ds(j * WIDE, WIDE)], wsem.at[j]) for j in range(tiles)]
    if not last:
        dq = wdq_hbm.shape[2]
        dkv = wdkv_hbm.shape[1]
        lat = kv_gain_ref.shape[1]
        dq_cp = [pltpu.make_async_copy(wdq_hbm.at[layer + 1, :, pl.ds(j * 256, 256)], wgu.at[:, pl.ds(j * 256, 256)], gsem.at[j]) for j in range(dq // 256)]
        dkv_cp = [pltpu.make_async_copy(wdkv_hbm.at[layer + 1], wod.at[pl.ds(0, dkv)], wsem.at[0])]
    pl.semaphore_wait(barrier, 3)

    def remote(kind, ph, r):
        dev = {'0': pair, '1': n1, '2': n2}[kind[1]] if kind[0] == 'S' else {'0': n2, '1': n1, '2': pair}[kind[1]]
        k = 6 * ph + ('S0', 'S1', 'S2', 'G0', 'G1', 'G2').index(kind)
        if kind == 'S0':
            src, dst = buf.at[r, pl.ds(al(half_oth), half)], r0.at[r % 2]
        elif kind == 'S1':
            src, dst = buf.at[r, pl.ds(al(quart_oth), quart)], r1.at[r]
        elif kind == 'S2':
            src, dst = buf.at[r, pl.ds(al(eig_oth), eighth)], r2.at[r]
        else:
            off, n = {'G0': (eig_own, eighth), 'G1': (quart_own, quart), 'G2': (half_own, half)}[kind]
            src = buf.at[r, pl.ds(al(off), n)]
            dst = src
        return pltpu.make_async_remote_copy(src_ref=src, dst_ref=dst, send_sem=ss.at[k, r], recv_sem=rs.at[k, r],
                                            device_id={'tp': dev}, device_id_type=MESH)

    def send(kind, ph, r):
        if kind == 'S0' and (ph, r) not in ((0, 0), (0, 1)):
            pl.semaphore_wait(credit, 1)
        remote(kind, ph, r).start()

    def landed(kind, ph, r, dev):
        remote(kind, ph, r).wait_recv()
        remote(kind, ph, r).wait_send()
        pl.semaphore_signal(ack.at[3 * ph + int(kind[1]), r], inc=1, device_id={'tp': dev}, device_id_type=MESH)

    def granted(kind, ph, r):
        pl.semaphore_wait(ack.at[3 * ph + int(kind[1]), r], 1)

    def add_rows(r, off, src, src_off, n, slot):
        def tile(t, _):
            cs = pl.ds(pl.multiple_of(t * WIDE, WIDE), WIDE)
            rw = pl.ds(al(off), n)
            buf[r, rw, cs] = (buf[r, rw, cs].astype(F32) + src[slot, pl.ds(al(src_off), n), cs].astype(F32)).astype(BF)
            return 0
        lax.fori_loop(0, tiles, tile, 0)

    def out_copy(r):
        return pltpu.make_async_copy(buf.at[r], out_hbm.at[r], osem.at[r])

    def step_o(r):
        if r == 0:
            for cp in x_cp:
                cp.wait()

        def tile(t, _):
            if r == 0:
                pltpu.make_async_copy(wo_hbm.at[layer, :, pl.ds(0, WIDE)], wod.at[pl.ds(0, depth), pl.ds(0, WIDE)], wsem.at[t]).wait()
            cs = pl.ds(pl.multiple_of(t * WIDE, WIDE), WIDE)
            buf[r, :, cs] = jnp.dot(act[:, 0:depth], wod[0:depth, cs], preferred_element_type=F32).astype(BF)
            return 0
        lax.fori_loop(0, tiles, tile, 0)
        send('S0', 0, r)

    def step_m(m):
        r = m // SUBS
        part = lax.rem(m, SUBS)
        n_gate = cols // 128 // 3

        def gate(j, _):
            @pl.when(r == 0)
            def _():
                for i in range(2):
                    pltpu.make_async_copy(wg_hbm.at[layer, :, pl.ds(0, 128)], wgu.at[:, pl.ds(0, 128)], gsem.at[2 * j + i]).wait()
            cs = pl.ds(pl.multiple_of(j * 256, 256), 256)
            pre = jnp.dot(buf[r], wgu[:, cs], preferred_element_type=F32)
            act[:, pl.ds(pl.multiple_of(j * 128, 128), 128)] = (jax.nn.silu(pre[:, :128]) * pre[:, 128:]).astype(BF)
            return 0

        def tile(t, _):
            cs = pl.ds(pl.multiple_of(t * WIDE, WIDE), WIDE)
            buf[r, :, cs] = jnp.dot(act[...], wod[:, cs], preferred_element_type=F32).astype(BF)
            return 0

        @pl.when(part < 3)
        def _():
            lax.fori_loop(part * n_gate, (part + 1) * n_gate, gate, 0)

        @pl.when(m == 3)
        def _():
            wait_all(wd_cp)

        @pl.when(part == 3)
        def _():
            for kind in ('G0', 'G1', 'G2'):
                remote(kind, 0, r).wait_send()

        @pl.when(part >= 3)
        def _():
            cut = (tiles + 1) // 2
            lax.fori_loop((part - 3) * cut, cut + (part - 3) * (tiles - cut), tile, 0)

    def reduce_own(ph, r):
        def tile(t, acc):
            cs = pl.ds(pl.multiple_of(t * WIDE, WIDE), WIDE)
            v = own[r, :, cs].astype(F32) + (buf[r, pl.ds(al(eig_own), eighth), cs].astype(F32) + r2[r, :, cs].astype(F32))
            v = v.astype(BF)
            own[r, :, cs] = v
            if ph == 1 and last:
                buf[r, pl.ds(al(eig_own), eighth), cs] = v
            v = v.astype(F32)
            return acc + v * v
        acc = lax.fori_loop(0, tiles, tile, jnp.zeros((eighth, WIDE), F32))
        return lax.rsqrt(jnp.sum(acc, axis=-1, keepdims=True) * (1.0 / width) + NORM_EPS)

    def norm_own(r, inv, gain, put):
        def tile(t, _):
            cs = pl.ds(pl.multiple_of(t * WIDE, WIDE), WIDE)
            put(r, cs, (own[r, :, cs].astype(F32) * inv * gain[:, cs].astype(F32)).astype(BF))
            return 0
        lax.fori_loop(0, tiles, tile, 0)

    def put_buf(r, cs, v):
        buf[r, pl.ds(al(eig_own), eighth), cs] = v

    def put_r2(r, cs, v):
        r2[r, :, cs] = v

    def step_t(k):
        rows_n = STEP * heads
        nsub = STEP // SUB
        wait_all(q_copies(k))
        q_row, q_col = q_at(k)
        qr_cols = [pl.ds(pl.multiple_of((2 * k + i) * 128, 128), 128) for i in range(2)]
        for i in range(STEP):
            posv[i * heads:(i + 1) * heads, :] = jnp.full((heads, 128), pos_ref[k * STEP + i], jnp.int32)
        slots = []
        for j in range(nsub):
            t = k * nsub + j
            wait_all(cache_copies(t))
            slot = lax.rem(t, SLOTS)
            row, col = slot_at(slot)
            slots.append((row, col))
            k_row = pl.multiple_of(slot * (SUB * n_rope), SUB * n_rope)
            for e in range(SUB):
                i = j * SUB + e
                lo = i // 2 * 16
                up = i % 2 * heads
                keys_i = wgu[pl.ds(row + e * keys, keys), pl.ds(col, n_lat)]
                s_i = lax.dot_general(wgu[pl.ds(q_row + lo, 16), pl.ds(q_col, n_lat)], keys_i, NT, preferred_element_type=F32)
                s_i = s_i + jnp.dot(wod[depth + lo % 128:depth + lo % 128 + 16, qr_cols[lo // 128]][:, :n_rope], wgu[pl.ds(k_row + e * n_rope, n_rope), pl.ds(k_col, keys)], preferred_element_type=F32)
                sc[i * heads:(i + 1) * heads, :] = s_i[up:up + heads]
        seqs = pl.ds(pl.multiple_of(k * STEP, STEP), STEP)
        col_id = lax.broadcasted_iota(jnp.int32, (rows_n, keys), 1)
        pv = posv[:, 0:1]
        cn = cn_ref[seqs, :].astype(F32)
        kn = kn_ref[seqs, :].astype(F32)
        fresh = jnp.sum(wgu[pl.ds(q_row, rows_n), pl.ds(q_col, n_lat)].astype(F32) * jnp.broadcast_to(cn[:, None, :], (STEP, heads, n_lat)).reshape(rows_n, n_lat), axis=-1, keepdims=True)
        kn8 = jnp.broadcast_to(kn[:, None, :], (STEP, heads, 128)).reshape(rows_n, 128)
        fresh = fresh + jnp.sum(jnp.concatenate([wod[depth:depth + 128, cs].astype(F32) for cs in qr_cols], axis=0) * kn8, axis=-1, keepdims=True)
        hit = col_id == pv
        sco = jnp.where(hit, fresh, sc[...]) * scale
        sco = jnp.where(col_id <= pv, sco, -jnp.inf)
        e_x = jnp.exp(sco - jnp.max(sco, axis=-1, keepdims=True))
        w = (e_x / jnp.sum(e_x, axis=-1, keepdims=True)).astype(BF).astype(F32)
        new_prob = jnp.sum(jnp.where(hit, w, 0.0), axis=-1, keepdims=True)
        new_part = (new_prob.reshape(STEP, heads, 1) * cn[:, None, :]).reshape(rows_n, n_lat)
        for b in range(n_lat // 128):
            ctx[b] = new_part[:, b * 128:(b + 1) * 128]
        sc[...] = jnp.where(hit, 0.0, w)
        for j in range(nsub):
            row, col = slots[j]
            for e in range(SUB):
                rw = slice((j * SUB + e) * heads, (j * SUB + e + 1) * heads)
                val = jnp.dot(sc[rw, :].astype(BF), wgu[pl.ds(row + e * keys, keys), pl.ds(col, n_lat)], preferred_element_type=F32)
                for b in range(n_lat // 128):
                    ctx[b, rw, :] = (ctx[b, rw, :] + val[:, b * 128:(b + 1) * 128]).astype(BF).astype(F32)
            nxt = k * nsub + j + SLOTS

            @pl.when(nxt < total)
            def _():
                start_all(cache_copies(nxt))
        out_rows = pl.ds(pl.multiple_of(lax.rem(k, steps // CHUNKS) * STEP, STEP), STEP)
        for h in range(heads):
            ctx_h = jnp.concatenate([ctx[b, pl.ds(h, STEP, stride=heads), :] for b in range(n_lat // 128)], axis=1).astype(BF)
            act[out_rows, h * 128:(h + 1) * 128] = jnp.dot(ctx_h, uv_ref[:, h * 128:(h + 1) * 128], preferred_element_type=F32).astype(BF)

    def event(op, ph, r):
        if op == 'O':
            step_o(r)
        elif op == 'A0':
            landed('S0', ph, r, pair)
            add_rows(r, quart_oth, r0, (1 - f) * quart, quart, r % 2)
            add_rows(r, quart_own, r0, f * quart, quart, r % 2)
            if (ph, r) not in ((1, 2), (1, 3)):
                pl.semaphore_signal(credit, inc=1, device_id={'tp': pair}, device_id_type=MESH)
            send('S1', ph, r)
        elif op == 'A1':
            landed('S1', ph, r, n1)
            add_rows(r, eig_oth, r1, (1 - s) * eighth, eighth, r)
            add_rows(r, eig_own, r1, s * eighth, eighth, r)
            send('S2', ph, r)
        elif op == 'A2':
            landed('S2', ph, r, n2)
            inv = reduce_own(ph, r)
            if ph == 0:
                norm_own(r, inv, gain_ref, put_buf)
            elif not last:
                norm_own(r, inv, next_gain_ref, put_r2)
            if ph == 0 or last:
                granted('S2', ph, r)
                send('G0', ph, r)
        elif op == 'B0':
            remote('G0', ph, r).wait_recv()
            granted('S1', ph, r)
            send('G1', ph, r)
        elif op == 'B1':
            remote('G1', ph, r).wait_recv()
            granted('S0', ph, r)
            send('G2', ph, r)
        elif op == 'B2':
            remote('G2', ph, r).wait_recv()
            if ph == 1:
                out_copy(r).start()


    hooks = {'T': [[]], 'M': [[]]}
    now = 'T'
    for token in (ORDER_LAST if last else ORDER_MID):
        if token in hooks:
            now = token
            hooks[now].append([])
        else:
            hooks[now][-1].append((token[:-2], int(token[-2]), int(token[-1])))

    def run(name, step, k):
        step(k)
        for at, evs in enumerate(hooks[name][1:]):
            if evs or name == 'M':
                @pl.when(k == at)
                def _(at=at, evs=evs):
                    if name == 'M' and at % SUBS == SUBS - 1:
                        send('S0', 1, at // SUBS)
                        if at == SUBS * CHUNKS - 1 and not last:
                            start_all(dkv_cp)
                    if name == 'M' and at == SUBS * CHUNKS - 3 and not last:
                        start_all(dq_cp)
                    for ev in evs:
                        if ev[0] == 'O' and ev[2] == CHUNKS - 1:
                            start_all(gu_cp)
                        event(*ev)
                        if ev[0] == 'O' and ev[2] == CHUNKS - 1:
                            start_all(wd_cp)
        return 0
    lax.fori_loop(0, steps, lambda k, _: run('T', step_t, k), 0)
    lax.fori_loop(0, SUBS * CHUNKS, lambda k, _: run('M', step_m, k), 0)

    if last:
        for r in range(CHUNKS):
            for kind in ('G0', 'G1', 'G2'):
                remote(kind, 1, r).wait_send()
            out_copy(r).wait()
        return

    own_cp = pltpu.make_async_copy(own, own_out, osem.at[0])
    own_cp.start()
    n = CHUNKS * eighth
    mine = pl.ds(al(eig_own), eighth)
    def a():
        return r2[...].reshape(n, width)

    for cp in dkv_cp:
        cp.wait()
    kv = lax.dot_general(a(), wod[0:lat, :], NT, preferred_element_type=F32)
    inv = lax.rsqrt(jnp.mean(kv * kv, axis=-1, keepdims=True) + NORM_EPS)
    buf[:, mine, dq:dq + lat] = (kv * inv * kv_gain_ref[...].astype(F32)).astype(BF).reshape(CHUNKS, eighth, lat)
    kp = lax.dot_general(a(), wod[lat:lat + 128, :], NT, preferred_element_type=F32)
    rope = dkv - lat
    lane = lax.broadcasted_iota(jnp.int32, (n, 128), 1)
    swap = jnp.where(lane < rope // 2, pltpu.roll(kp, 128 - rope // 2, 1), pltpu.roll(kp, rope // 2, 1))
    kp = jnp.where(lane < rope, kp * cos_v[...].reshape(n, 128) + swap * sin_v[...].reshape(n, 128), 0.0)
    buf[:, mine, dq + lat:dq + lat + 128] = kp.astype(BF).reshape(CHUNKS, eighth, 128)
    for cp in dq_cp:
        cp.wait()
    total_sq = jnp.zeros((n, 1), F32)
    for j in range(dq // 512):
        v = jnp.dot(a(), wgu[:, j * 512:(j + 1) * 512], preferred_element_type=F32)
        total_sq = total_sq + jnp.sum(v * v, axis=-1, keepdims=True)
        for b in range(4):
            ctx[b, j * n:(j + 1) * n, :] = v[:, b * 128:(b + 1) * 128]
    inv = lax.rsqrt(total_sq * (1.0 / dq) + NORM_EPS)
    for j in range(dq // 128):
        cs = slice(j * 128, (j + 1) * 128)
        v = ctx[j % 4, j // 4 * n:(j // 4 + 1) * n, :]
        buf[:, mine, cs] = (v * inv * q_gain_ref[:, cs].astype(F32)).astype(BF).reshape(CHUNKS, eighth, 128)

    used = dq + lat + 128

    def gather(k, off, rows_n, dev):
        part = buf.at[:, pl.ds(al(off), rows_n), pl.ds(0, used)]
        cp = pltpu.make_async_remote_copy(src_ref=part, dst_ref=part, send_sem=ss.at[k, 0], recv_sem=rs.at[k, 0],
                                          device_id={'tp': dev}, device_id_type=MESH)
        cp.start()
        return cp

    for r in range(CHUNKS):
        granted('S2', 1, r)
    g0 = gather(9, eig_own, eighth, n2)
    g0.wait_recv()
    for r in range(CHUNKS):
        granted('S1', 1, r)
    g1 = gather(10, quart_own, quart, n1)
    g1.wait_recv()
    for r in range(CHUNKS):
        granted('S0', 1, r)
    g2 = gather(11, half_own, half, pair)
    g2.wait_recv()
    outs = [pltpu.make_async_copy(buf.at[:, :, pl.ds(0, dq)], cq_out, osem.at[1]),
            pltpu.make_async_copy(buf.at[:, :, pl.ds(dq, lat)], ckv_out, osem.at[2]),
            pltpu.make_async_copy(buf.at[:, :, pl.ds(dq + lat, 128)], kpe_out, osem.at[3])]
    for cp in outs:
        cp.start()
    for cp in (g0, g1, g2):
        cp.wait_send()
    own_cp.wait()
    for cp in outs:
        cp.wait()


def fused_layer(layer, last, scale, pos, c_new, k_new, w_uv, q_lat, q_rope, ckv, kpe_t, resid, mlp_gain, w_o, w_gate, w_up, w_down, more):
    n, width = c_new.shape[0], w_down.shape[2]
    lat = c_new.shape[1]
    keys = kpe_t.shape[2]
    rows = n // CHUNKS
    depth, cols = w_o.shape[1], w_down.shape[1]
    vm = pl.BlockSpec(memory_space=pltpu.VMEM)
    hb = pl.BlockSpec(memory_space=pl.ANY)
    args = [pos, c_new, k_new, w_uv, q_lat, q_rope, ckv, kpe_t, resid, mlp_gain, w_o, w_gate, w_up, w_down]
    specs = [pl.BlockSpec(memory_space=pltpu.SMEM), vm, vm, vm, hb, hb, hb, hb, hb, vm, hb, hb, hb, hb]
    scratch = [pltpu.VMEM((width, 2 * cols), BF), pltpu.VMEM((cols, width), BF), pltpu.VMEM((CHUNKS, rows, width), BF),
               pltpu.VMEM((2, rows // 2, width), BF), pltpu.VMEM((CHUNKS, rows // 4, width), BF),
               pltpu.VMEM((CHUNKS, rows // 8, width), BF), pltpu.VMEM((CHUNKS, rows // 8, width), BF),
               pltpu.VMEM((rows, cols), BF), pltpu.VMEM((STEP * 8, keys), F32), pltpu.VMEM((lat // 128, STEP * 8, 128), F32), pltpu.VMEM((STEP * 8, 128), jnp.int32)]
    if last:
        outs = jax.ShapeDtypeStruct((CHUNKS, rows, width), BF)
        out_specs = hb
    else:
        next_gain, q_gain, kv_gain, cos_t, sin_t, w_dq, w_dkv_t = more
        args += [next_gain, q_gain, kv_gain, cos_t, sin_t, w_dq, w_dkv_t]
        specs += [vm, vm, vm, hb, hb, hb, hb]
        outs = (jax.ShapeDtypeStruct((CHUNKS, rows // 8, width), BF), jax.ShapeDtypeStruct((CHUNKS, rows, w_dq.shape[2]), BF),
                jax.ShapeDtypeStruct((CHUNKS, rows, kv_gain.shape[1]), BF), jax.ShapeDtypeStruct((CHUNKS, rows, 128), BF))
        out_specs = (hb,) * 4
    scratch += [pltpu.SemaphoreType.DMA((width // WIDE,)), pltpu.SemaphoreType.DMA((2 * cols // 128,)),
                pltpu.SemaphoreType.DMA((3,)), pltpu.SemaphoreType.DMA((4,)),
                pltpu.SemaphoreType.DMA((12, CHUNKS)), pltpu.SemaphoreType.DMA((12, CHUNKS)),
                pltpu.SemaphoreType.REGULAR((6, CHUNKS)), pltpu.SemaphoreType.REGULAR, pltpu.SemaphoreType.DMA((SLOTS,)), pltpu.SemaphoreType.DMA((SLOTS,)),
                pltpu.SemaphoreType.DMA((n // STEP,)), pltpu.SemaphoreType.DMA((2 * n // STEP,))]
    if not last:
        scratch += [pltpu.VMEM((CHUNKS, rows // 8, 128), F32)] * 2
    return pl.pallas_call(
        functools.partial(layer_body, layer, last, scale), in_specs=specs, out_specs=out_specs, out_shape=outs, scratch_shapes=scratch,
        name='layer_last' if last else 'layer_mid',
        compiler_params=pltpu.CompilerParams(collective_id=1 if last else 0, has_side_effects=True, vmem_limit_bytes=67043328),
        cost_estimate=pl.CostEstimate(flops=2 * n * (width * (depth + 3 * cols) + 8 * keys * 2 * lat), bytes_accessed=2 * width * (depth + 3 * cols) + 2 * n * keys * lat, transcendentals=n * cols),
    )(*args)


def solution(mesh):
    cache_spec = P(None, 'dp', None, None)
    head_spec = P(None, None, 'tp', None)
    weight_specs = (P(), P(), P(), P(), P(), head_spec, head_spec, head_spec, P(None, 'tp', None, None), P(), P(None, None, 'tp'), P(None, None, 'tp'), P(None, 'tp', None))
    in_specs = (P('dp', None), P('dp'), cache_spec, cache_spec) + weight_specs
    out_specs = (P('dp', None), P(None, 'dp', None), P(None, 'dp', None))

    def device_body(x_in, pos_ids, ckv_cache, kpe_cache, attn_gain, w_dq, q_gain, w_dkv, kv_gain, w_uq, w_uk, w_uv, w_o, mlp_gain, w_gate, w_up, w_down):
        n, width = x_in.shape
        rows = n // CHUNKS
        lat = w_uk.shape[1]
        nope = w_uk.shape[3]
        rope = kpe_cache.shape[3]
        half = rope // 2
        inv_freq = jnp.exp(jnp.arange(half, dtype=F32) * (-2.0 * math.log(ROPE_BASE) / rope))
        angles = pos_ids.astype(F32)[:, None] * inv_freq
        cos_p, sin_p = jnp.cos(angles), jnp.sin(angles)
        pad = jnp.zeros((n, 128 - rope), F32)
        cos_t = jnp.concatenate([cos_p, cos_p, pad], axis=1).reshape(CHUNKS, rows, 128)
        sin_t = jnp.concatenate([-sin_p, sin_p, pad], axis=1).reshape(CHUNKS, rows, 128)
        kpe_t = jnp.swapaxes(kpe_cache, 2, 3)
        w_dkv_t = jnp.swapaxes(w_dkv, 1, 2)
        w_o2 = w_o.reshape(w_o.shape[0], -1, width)
        scale = w_uq.shape[-1] ** -0.5

        ckv_2d = ckv_cache.reshape(ckv_cache.shape[0], -1, lat)
        kpe_2d = kpe_t.reshape(kpe_t.shape[0], -1, kpe_t.shape[3])

        def heads_of(layer, c_q):
            q_full = jnp.einsum('bc,chd->bhd', c_q, w_uq[layer], preferred_element_type=F32)
            q_nope = q_full[..., :nope].astype(BF)
            q_rope = rotate(q_full[..., nope:], cos_p[:, None], sin_p[:, None]).astype(BF)
            q_lat = jnp.einsum('bhn,chn->bhc', q_nope, w_uk[layer], preferred_element_type=F32).astype(BF)
            q_rope = jnp.pad(q_rope, ((0, 0), (0, 0), (0, 128 - rope)))
            return w_uv[layer].reshape(lat, -1), q_lat.reshape(-1, lat), q_rope.reshape(-1, 128), ckv_2d, kpe_2d

        normed = rms_norm(x_in, attn_gain[0])
        c_q = rms_norm(jnp.dot(normed, w_dq[0], preferred_element_type=F32), q_gain[0])
        kv = jnp.dot(normed, w_dkv[0], preferred_element_type=F32)
        c_new0 = rms_norm(kv[:, :lat], kv_gain[0])
        k_new0 = rotate(kv[:, lat:], cos_p, sin_p).astype(BF)
        k_pad0 = jnp.pad(k_new0, ((0, 0), (0, 128 - rope)))
        x_own, c_q, c_new1, k_pad1 = fused_layer(
            0, False, scale, pos_ids, c_new0, k_pad0, *heads_of(0, c_q), x_in.reshape(CHUNKS, rows, width), mlp_gain[0:1], w_o2, w_gate, w_up, w_down,
            (attn_gain[1:2], q_gain[1:2], kv_gain[1:2], cos_t, sin_t, w_dq, w_dkv_t))
        c_new1 = c_new1.reshape(n, lat)
        k_pad1 = k_pad1.reshape(n, 128)
        k_new1 = k_pad1[:, :rope]
        x_out = fused_layer(1, True, scale, pos_ids, c_new1, k_pad1, *heads_of(1, c_q.reshape(n, -1)), x_own, mlp_gain[1:2], w_o2, w_gate, w_up, w_down, None)
        return x_out.reshape(n, width), jnp.stack([c_new0, c_new1]), jnp.stack([k_new0, k_new1])

    return jax.shard_map(device_body, mesh=mesh, in_specs=in_specs, out_specs=out_specs, check_vma=False)
```

```python
import functools
import math
import jax
import jax.numpy as jnp
from jax import lax
from jax.experimental import pallas as pl
from jax.experimental.pallas import tpu as pltpu
from jax.sharding import PartitionSpec as P

NORM_EPS = 1e-6
ROPE_BASE = 10000.0
BF = jnp.bfloat16
F32 = jnp.float32
NT = (((1,), (1,)), ((), ()))
MESH = pl.DeviceIdType.MESH

SUB = 8
LANES = 128
STEP = 16
SUBS = 5
SLOTS = 9
CHUNKS = 4
WIDE = 1024

ORDER_LAST = (
    'T', 'T', 'T', 'T', 'E00', 'T', 'T', 'O00', 'T', 'T', 'A000', 'E01', 'T', 'T',
    'O01', 'T', 'A100', 'T', 'A001', 'E02', 'T', 'A200', 'O02', 'T', 'A101', 'T', 'B000', 'A002',
    'T', 'E03', 'A201', 'O03', 'B100', 'B001', 'A003', 'B200', 'M', 'A102', 'M', 'M', 'B101', 'M',
    'A202', 'M', 'B201', 'M', 'A103', 'M', 'B002', 'A010', 'M', 'M', 'A203', 'M', 'B102', 'A011',
    'B003', 'B202', 'M', 'A110', 'M', 'M', 'M', 'A210', 'A111', 'M', 'B103', 'A012', 'B010', 'B203',
    'M', 'A211', 'M', 'M', 'A112', 'M', 'B011', 'M', 'B110', 'A212', 'A013', 'B210', 'B111', 'B012',
    'B211', 'A113', 'B112', 'A213', 'B212', 'B013', 'B113', 'B213',
)
ORDER_MID = (
    'T', 'T', 'T', 'T', 'E00', 'T', 'O00', 'T', 'T', 'A000', 'T', 'E01', 'T', 'O01',
    'T', 'A100', 'T', 'A001', 'T', 'E02', 'T', 'A200', 'O02', 'T', 'A101', 'T', 'B000', 'A002',
    'T', 'E03', 'A201', 'O03', 'B100', 'A003', 'B001', 'B200', 'M', 'M', 'A102', 'M', 'M', 'M',
    'A103', 'A202', 'A010', 'B101', 'A203', 'B201', 'M', 'M', 'B002', 'A110', 'M', 'M', 'B003', 'M',
    'A210', 'B102', 'A011', 'B202', 'M', 'M', 'B103', 'M', 'M', 'B203', 'M', 'A111', 'M', 'M',
    'A012', 'M', 'A211', 'M', 'M', 'A112', 'A013', 'A212', 'A113', 'A213',
)


def rms_norm(values, norm_gain):
    values = values.astype(F32)
    inv_rms = lax.rsqrt(jnp.mean(values * values, axis=-1, keepdims=True) + NORM_EPS)
    return (values * inv_rms * norm_gain.astype(F32)).astype(BF)


def rotate(values, cos_part, sin_part):
    half_dim = values.shape[-1] // 2
    lo_half = values[..., :half_dim]
    hi_half = values[..., half_dim:]
    return jnp.concatenate([lo_half * cos_part - hi_half * sin_part, hi_half * cos_part + lo_half * sin_part], axis=-1)


def layer_body(layer, last, scale, *refs):
    (pos_ref, cn_ref, kn_ref, uva_hbm, uvb_hbm, qa_hbm, qb_hbm, ra_hbm, rb_hbm, ckv_hbm, kpe_hbm, x_hbm, gain_ref, wo_hbm, wg_hbm, wu_hbm, wd_hbm), refs = refs[:17], refs[17:]
    if last:
        out_hbm, refs = refs[0], refs[1:]
    else:
        (next_gain_ref, q_gain_ref, kv_gain_ref, cos_hbm, sin_hbm, wdq_hbm, wdkv_hbm, own_out, cq_out, ckv_out, kpe_out), refs = refs[:11], refs[11:]
    (wgu, wod, buf, r0, r1, r2, own, act, sc, ctx, posv, rope_t, fresh_v, wsem, gsem, xsem, osem, ss, rs, ack, credit, csem, ksem, qsem, uvsem, es, er), refs = refs[:27], refs[27:]
    if not last:
        cos_v, sin_v = refs
    heads = 16
    own_heads = 8
    keys = sc.shape[1]
    n_lat = qa_hbm.shape[2]
    n_rope = kpe_hbm.shape[1] // (ckv_hbm.shape[1] // keys)
    steps = qa_hbm.shape[0]
    per = steps // CHUNKS
    total = steps * (STEP // SUB)
    blk = STEP * own_heads
    q_base = 3 * SUB * keys
    k_col = 4 * n_lat
    v_col = 3 * n_lat
    c_row = 4 * n_lat
    c_rows = STEP * per
    send_row = c_row + heads * c_rows
    ho_row = send_row + 2 * CHUNKS * c_rows
    depth = wo_hbm.shape[1]
    cols = wd_hbm.shape[1]
    width = wd_hbm.shape[2]
    rows = buf.shape[1]
    half, quart, eighth = rows // 2, rows // 4, rows // 8
    tiles = width // WIDE

    me = lax.axis_index('tp')
    c = lax.rem(me, 2)
    x = lax.rem(me // 2, 2)
    y = me // 4
    f = x * (1 - c) + y * c
    s = y * (1 - c) + x * c
    pair = y * 4 + x * 2 + (1 - c)
    n1 = (y * (1 - c) + (1 - y) * c) * 4 + ((1 - x) * (1 - c) + x * c) * 2 + c
    n2 = ((1 - y) * (1 - c) + y * c) * 4 + (x * (1 - c) + (1 - x) * c) * 2 + c
    half_own, half_oth = c * half, (1 - c) * half
    quart_own, quart_oth = half_own + f * quart, half_own + (1 - f) * quart
    eig_own, eig_oth = quart_own + s * eighth, quart_own + (1 - s) * eighth
    al = lambda v: pl.multiple_of(v, 16)

    barrier = pltpu.get_barrier_semaphore()
    for dev in (pair, n1, n2):
        pl.semaphore_signal(barrier, inc=1, device_id={'tp': dev}, device_id_type=MESH)

    def slot_at(slot):
        return pl.multiple_of(lax.rem(slot, 3) * (SUB * keys), SUB * keys), pl.multiple_of(slot // 3 * n_lat, n_lat)

    def cache_copies(t):
        slot = lax.rem(t, SLOTS)
        row, col = slot_at(slot)
        sub = STEP // SUB
        first = t // (per * sub) * rows + c * half + lax.rem(t, per * sub) * SUB
        return (pltpu.make_async_copy(ckv_hbm.at[layer, pl.ds(pl.multiple_of(first * keys, SUB * keys), SUB * keys)],
                                      wgu.at[pl.ds(row, SUB * keys), pl.ds(col, n_lat)], csem.at[slot]),
                pltpu.make_async_copy(kpe_hbm.at[layer, pl.ds(pl.multiple_of(first * n_rope, SUB * n_rope), SUB * n_rope)],
                                      wgu.at[pl.ds(pl.multiple_of(slot * (SUB * n_rope), SUB * n_rope), SUB * n_rope), pl.ds(k_col, keys)], ksem.at[slot]))

    def q_at(k):
        return pl.multiple_of(q_base + lax.rem(k, 4) * (STEP * heads), STEP * heads), pl.multiple_of(k // 4 * n_lat, n_lat)

    def q_copies(k):
        row, col = q_at(k)
        out = []
        for i, (lat_hbm, rope_hbm) in enumerate(((qa_hbm, ra_hbm), (qb_hbm, rb_hbm))):
            out.append(pltpu.make_async_copy(lat_hbm.at[k], wgu.at[pl.ds(row + i * blk, blk), pl.ds(col, n_lat)], qsem.at[k, 2 * i]))
            out.append(pltpu.make_async_copy(rope_hbm.at[k], wod.at[pl.ds(depth, LANES), pl.ds(pl.multiple_of((2 * k + i) * LANES, LANES), LANES)], qsem.at[k, 2 * i + 1]))
        return out

    uv_cp = []
    for i, uv_hbm in enumerate((uva_hbm, uvb_hbm)):
        for b in range(2):
            uv_cp.append(pltpu.make_async_copy(uv_hbm.at[layer, :, pl.ds(b * n_lat, n_lat)], wgu.at[pl.ds((2 * i + b) * n_lat, n_lat), pl.ds(v_col, n_lat)], uvsem.at[2 * i + b]))

    def start_all(cps):
        for cp in cps:
            cp.start()

    def wait_all(cps):
        for cp in cps:
            cp.wait()

    start_all(q_copies(0))
    for t in range(STEP // SUB):
        start_all(cache_copies(t))
    start_all(q_copies(1))
    for t in range(STEP // SUB, SLOTS):
        start_all(cache_copies(t))

    def more_q(k, _):
        start_all(q_copies(k))
        return 0
    lax.fori_loop(2, steps, more_q, 0)
    start_all(uv_cp)

    wo_cp = [pltpu.make_async_copy(wo_hbm.at[layer, :, pl.ds(j * WIDE, WIDE)], wod.at[pl.ds(0, depth), pl.ds(j * WIDE, WIDE)], wsem.at[j]) for j in range(tiles)]
    for cp in wo_cp:
        cp.start()
    if last:
        x_cp = [pltpu.make_async_copy(x_hbm, own, xsem.at[0])]
    else:
        x_cp = [pltpu.make_async_copy(x_hbm.at[:, pl.ds(al(eig_own), eighth)], own, xsem.at[0]),
                pltpu.make_async_copy(cos_hbm.at[:, pl.ds(al(eig_own), eighth)], cos_v, xsem.at[1]),
                pltpu.make_async_copy(sin_hbm.at[:, pl.ds(al(eig_own), eighth)], sin_v, xsem.at[2])]
    for cp in x_cp:
        cp.start()
    gu_cp = []
    for j in range(cols // LANES):
        gu_cp.append(pltpu.make_async_copy(wg_hbm.at[layer, :, pl.ds(j * LANES, LANES)], wgu.at[:, pl.ds(2 * j * LANES, LANES)], gsem.at[2 * j]))
        gu_cp.append(pltpu.make_async_copy(wu_hbm.at[layer, :, pl.ds(j * LANES, LANES)], wgu.at[:, pl.ds((2 * j + 1) * LANES, LANES)], gsem.at[2 * j + 1]))
    wd_cp = [pltpu.make_async_copy(wd_hbm.at[layer, :, pl.ds(j * WIDE, WIDE)], wod.at[:, pl.ds(j * WIDE, WIDE)], wsem.at[j]) for j in range(tiles)]
    if not last:
        dq = wdq_hbm.shape[2]
        dkv = wdkv_hbm.shape[1]
        lat = kv_gain_ref.shape[1]
        dq_cp = [pltpu.make_async_copy(wdq_hbm.at[layer + 1, :, pl.ds(j * 256, 256)], wgu.at[:, pl.ds(j * 256, 256)], gsem.at[j]) for j in range(dq // 256)]
        dkv_cp = [pltpu.make_async_copy(wdkv_hbm.at[layer + 1], wod.at[pl.ds(0, dkv)], wsem.at[0])]
    pl.semaphore_wait(barrier, 3)

    def remote(kind, ph, r):
        dev = {'0': pair, '1': n1, '2': n2}[kind[1]] if kind[0] == 'S' else {'0': n2, '1': n1, '2': pair}[kind[1]]
        k = 6 * ph + ('S0', 'S1', 'S2', 'G0', 'G1', 'G2').index(kind)
        if kind == 'S0':
            src, dst = buf.at[r, pl.ds(al(half_oth), half)], r0.at[r % 2]
        elif kind == 'S1':
            src, dst = buf.at[r, pl.ds(al(quart_oth), quart)], r1.at[r]
        elif kind == 'S2':
            src, dst = buf.at[r, pl.ds(al(eig_oth), eighth)], r2.at[r]
        else:
            off, n = {'G0': (eig_own, eighth), 'G1': (quart_own, quart), 'G2': (half_own, half)}[kind]
            src = buf.at[r, pl.ds(al(off), n)]
            dst = src
        return pltpu.make_async_remote_copy(src_ref=src, dst_ref=dst, send_sem=ss.at[k, r], recv_sem=rs.at[k, r],
                                            device_id={'tp': dev}, device_id_type=MESH)

    def send(kind, ph, r):
        if kind == 'S0' and (ph, r) not in ((0, 0), (0, 1)):
            pl.semaphore_wait(credit, 1)
        remote(kind, ph, r).start()

    def landed(kind, ph, r, dev):
        remote(kind, ph, r).wait_recv()
        remote(kind, ph, r).wait_send()
        pl.semaphore_signal(ack.at[3 * ph + int(kind[1]), r], inc=1, device_id={'tp': dev}, device_id_type=MESH)

    def granted(kind, ph, r):
        pl.semaphore_wait(ack.at[3 * ph + int(kind[1]), r], 1)

    def add_rows(r, off, src, src_off, n, slot):
        def tile(t, _):
            cs = pl.ds(pl.multiple_of(t * WIDE, WIDE), WIDE)
            rw = pl.ds(al(off), n)
            buf[r, rw, cs] = (buf[r, rw, cs].astype(F32) + src[slot, pl.ds(al(src_off), n), cs].astype(F32)).astype(BF)
            return 0
        lax.fori_loop(0, tiles, tile, 0)

    def out_copy(r):
        return pltpu.make_async_copy(buf.at[r], out_hbm.at[r], osem.at[r])

    def pair_copy(r, q):
        src = wgu.at[pl.ds(send_row + (2 * r + q) * c_rows, c_rows), pl.ds(v_col, n_lat)]
        dst = wgu.at[pl.ds(al(ho_row + (2 * r + q) * rows + c * c_rows), c_rows), pl.ds(v_col, n_lat)]
        return pltpu.make_async_remote_copy(src_ref=src, dst_ref=dst, send_sem=es.at[q, r], recv_sem=er.at[q, r],
                                            device_id={'tp': pair}, device_id_type=MESH)

    def step_e(r):
        if r == 0:
            wait_all(uv_cp)
        for own_side in (False, True):
            for h in range(own_heads):
                g = h if own_side else h + own_heads
                val = jnp.dot(wgu[c_row + g * c_rows:c_row + (g + 1) * c_rows, v_col:v_col + n_lat],
                              wgu[g // 4 * n_lat:(g // 4 + 1) * n_lat, v_col + g % 4 * LANES:v_col + (g % 4 + 1) * LANES], preferred_element_type=F32).astype(BF)
                cs = slice(v_col + h % 4 * LANES, v_col + (h % 4 + 1) * LANES)
                if own_side:
                    wgu[pl.ds(al(ho_row + (2 * r + h // 4) * rows + c * c_rows), c_rows), cs] = val
                else:
                    wgu[send_row + (2 * r + h // 4) * c_rows:send_row + (2 * r + h // 4 + 1) * c_rows, cs] = val
        for q in range(2):
            pair_copy(r, q).start()

    def step_o(r):
        for q in range(2):
            pair_copy(r, q).wait_recv()
            pair_copy(r, q).wait_send()
        if r == 0:
            for cp in x_cp:
                cp.wait()

        def tile(t, _):
            if r == 0:
                pltpu.make_async_copy(wo_hbm.at[layer, :, pl.ds(0, WIDE)], wod.at[pl.ds(0, depth), pl.ds(0, WIDE)], wsem.at[t]).wait()
            cs = pl.ds(pl.multiple_of(t * WIDE, WIDE), WIDE)
            acc = sum(jnp.dot(wgu[ho_row + (2 * r + q) * rows:ho_row + (2 * r + q + 1) * rows, v_col:v_col + n_lat], wod[q * n_lat:(q + 1) * n_lat, cs], preferred_element_type=F32) for q in range(2))
            buf[r, :, cs] = acc.astype(BF)
            return 0
        lax.fori_loop(0, tiles, tile, 0)
        send('S0', 0, r)

    def step_m(m):
        r = m // SUBS
        part = lax.rem(m, SUBS)
        n_gate = cols // LANES // 3

        def gate(j, _):
            @pl.when(r == 0)
            def _():
                for i in range(2):
                    pltpu.make_async_copy(wg_hbm.at[layer, :, pl.ds(0, LANES)], wgu.at[:, pl.ds(0, LANES)], gsem.at[2 * j + i]).wait()
            cs = pl.ds(pl.multiple_of(j * 256, 256), 256)
            pre = jnp.dot(buf[r], wgu[:, cs], preferred_element_type=F32)
            act[:, pl.ds(pl.multiple_of(j * LANES, LANES), LANES)] = (jax.nn.silu(pre[:, :LANES]) * pre[:, LANES:]).astype(BF)
            return 0

        def tile(t, _):
            cs = pl.ds(pl.multiple_of(t * WIDE, WIDE), WIDE)
            buf[r, :, cs] = jnp.dot(act[...], wod[:, cs], preferred_element_type=F32).astype(BF)
            return 0

        @pl.when(part < 3)
        def _():
            lax.fori_loop(part * n_gate, (part + 1) * n_gate, gate, 0)

        @pl.when(m == 3)
        def _():
            wait_all(wd_cp)

        @pl.when(part == 3)
        def _():
            for kind in ('G0', 'G1', 'G2'):
                remote(kind, 0, r).wait_send()

        @pl.when(part >= 3)
        def _():
            cut = (tiles + 1) // 2
            lax.fori_loop((part - 3) * cut, cut + (part - 3) * (tiles - cut), tile, 0)

    def reduce_own(ph, r):
        def tile(t, acc):
            cs = pl.ds(pl.multiple_of(t * WIDE, WIDE), WIDE)
            v = own[r, :, cs].astype(F32) + (buf[r, pl.ds(al(eig_own), eighth), cs].astype(F32) + r2[r, :, cs].astype(F32))
            v = v.astype(BF)
            own[r, :, cs] = v
            if ph == 1 and last:
                buf[r, pl.ds(al(eig_own), eighth), cs] = v
            v = v.astype(F32)
            return acc + v * v
        acc = lax.fori_loop(0, tiles, tile, jnp.zeros((eighth, WIDE), F32))
        return lax.rsqrt(jnp.sum(acc, axis=-1, keepdims=True) * (1.0 / width) + NORM_EPS)

    def norm_own(r, inv, gain, put):
        def tile(t, _):
            cs = pl.ds(pl.multiple_of(t * WIDE, WIDE), WIDE)
            put(r, cs, (own[r, :, cs].astype(F32) * inv * gain[:, cs].astype(F32)).astype(BF))
            return 0
        lax.fori_loop(0, tiles, tile, 0)

    def put_buf(r, cs, v):
        buf[r, pl.ds(al(eig_own), eighth), cs] = v

    def put_r2(r, cs, v):
        r2[r, :, cs] = v

    def step_t(k):
        rows_n = STEP * heads
        nsub = STEP // SUB
        wait_all(q_copies(k))
        q_row, q_col = q_at(k)
        blocks = [(slice(b * LANES, (b + 1) * LANES), pl.ds(pl.multiple_of(q_col + b * LANES, LANES), LANES)) for b in range(n_lat // LANES)]
        for b, (_, cs) in enumerate(blocks):
            ctx[b] = wgu[pl.ds(q_row, rows_n), cs].astype(F32)
        for i in range(2):
            rope_t[i * blk:(i + 1) * blk, :] = wod[depth:depth + LANES, pl.ds(pl.multiple_of((2 * k + i) * LANES, LANES), LANES)].astype(F32)
        cn = cn_ref[pl.ds(pl.multiple_of(k * STEP, STEP), STEP), :].astype(F32)
        kn = kn_ref[pl.ds(pl.multiple_of(k * STEP, STEP), STEP), :].astype(F32)
        slots = []
        for j in range(nsub):
            t = k * nsub + j
            wait_all(cache_copies(t))
            slot = lax.rem(t, SLOTS)
            row, col = slot_at(slot)
            slots.append((row, col))
            k_row = pl.multiple_of(slot * (SUB * n_rope), SUB * n_rope)
            for e in range(SUB):
                i = j * SUB + e
                q = jnp.concatenate([ctx[b, pl.ds(i, heads, stride=STEP), :] for b in range(n_lat // LANES)], axis=1)
                qr = rope_t[pl.ds(i, heads, stride=STEP), :]
                s_i = lax.dot_general(q.astype(BF), wgu[pl.ds(row + e * keys, keys), pl.ds(col, n_lat)], NT, preferred_element_type=F32)
                s_i = s_i + jnp.dot(qr[:, :n_rope].astype(BF), wgu[pl.ds(k_row + e * n_rope, n_rope), pl.ds(k_col, keys)], preferred_element_type=F32)
                sc[i * heads:(i + 1) * heads, :] = s_i
                part = qr * kn[i:i + 1]
                for b, (lo, _) in enumerate(blocks):
                    part = part + q[:, lo] * cn[i:i + 1, lo]
                fresh_v[i * heads:(i + 1) * heads, :] = part
                posv[i * heads:(i + 1) * heads, :] = jnp.full((heads, LANES), pos_ref[k * STEP + i], jnp.int32)
        col_id = lax.broadcasted_iota(jnp.int32, (rows_n, keys), 1)
        pv = posv[:, 0:1]
        fresh = jnp.sum(fresh_v[...], axis=-1, keepdims=True)
        hit = col_id == pv
        sco = jnp.where(hit, fresh, sc[...]) * scale
        sco = jnp.where(col_id <= pv, sco, -jnp.inf)
        e_x = jnp.exp(sco - jnp.max(sco, axis=-1, keepdims=True))
        w = (e_x / jnp.sum(e_x, axis=-1, keepdims=True)).astype(BF).astype(F32)
        fresh_v[...] = jnp.broadcast_to(jnp.sum(jnp.where(hit, w, 0.0), axis=-1, keepdims=True), fresh_v.shape)
        sc[...] = jnp.where(hit, 0.0, w)
        for j in range(nsub):
            row, col = slots[j]
            for e in range(SUB):
                i = j * SUB + e
                rw = slice(i * heads, (i + 1) * heads)
                val = jnp.dot(sc[rw, :].astype(BF), wgu[pl.ds(row + e * keys, keys), pl.ds(col, n_lat)], preferred_element_type=F32)
                for b, (lo, _) in enumerate(blocks):
                    ctx[b, rw, :] = val[:, lo] + fresh_v[rw, :] * cn[i:i + 1, lo]
            nxt = k * nsub + j + SLOTS

            @pl.when(nxt < total)
            def _():
                start_all(cache_copies(nxt))
        for h in range(heads):
            ctx_h = jnp.concatenate([ctx[b, pl.ds(h, STEP, stride=heads), :] for b in range(n_lat // LANES)], axis=1)
            wgu[pl.ds(al(c_row + h * c_rows + lax.rem(k, per) * STEP), STEP), v_col:v_col + n_lat] = ctx_h.astype(BF)

    def event(op, ph, r):
        if op == 'E':
            step_e(r)
        elif op == 'O':
            step_o(r)
        elif op == 'A0':
            landed('S0', ph, r, pair)
            add_rows(r, quart_oth, r0, (1 - f) * quart, quart, r % 2)
            add_rows(r, quart_own, r0, f * quart, quart, r % 2)
            if (ph, r) not in ((1, 2), (1, 3)):
                pl.semaphore_signal(credit, inc=1, device_id={'tp': pair}, device_id_type=MESH)
            send('S1', ph, r)
        elif op == 'A1':
            landed('S1', ph, r, n1)
            add_rows(r, eig_oth, r1, (1 - s) * eighth, eighth, r)
            add_rows(r, eig_own, r1, s * eighth, eighth, r)
            send('S2', ph, r)
        elif op == 'A2':
            landed('S2', ph, r, n2)
            inv = reduce_own(ph, r)
            if ph == 0:
                norm_own(r, inv, gain_ref, put_buf)
            elif not last:
                norm_own(r, inv, next_gain_ref, put_r2)
            if ph == 0 or last:
                granted('S2', ph, r)
                send('G0', ph, r)
        elif op == 'B0':
            remote('G0', ph, r).wait_recv()
            granted('S1', ph, r)
            send('G1', ph, r)
        elif op == 'B1':
            remote('G1', ph, r).wait_recv()
            granted('S0', ph, r)
            send('G2', ph, r)
        elif op == 'B2':
            remote('G2', ph, r).wait_recv()
            if ph == 1:
                out_copy(r).start()


    hooks = {'T': [[]], 'M': [[]]}
    now = 'T'
    for token in (ORDER_LAST if last else ORDER_MID):
        if token in hooks:
            now = token
            hooks[now].append([])
        else:
            hooks[now][-1].append((token[:-2], int(token[-2]), int(token[-1])))

    def run(name, step, k):
        step(k)
        for at, evs in enumerate(hooks[name][1:]):
            if evs or name == 'M':
                @pl.when(k == at)
                def _(at=at, evs=evs):
                    if name == 'M' and at % SUBS == SUBS - 1:
                        send('S0', 1, at // SUBS)
                        if at == SUBS * CHUNKS - 1 and not last:
                            start_all(dkv_cp)
                    if name == 'M' and at == SUBS * CHUNKS - 3 and not last:
                        start_all(dq_cp)
                    for ev in evs:
                        if ev[0] == 'O' and ev[2] == CHUNKS - 1:
                            start_all(gu_cp[:v_col // LANES] + gu_cp[k_col // LANES:])
                        event(*ev)
                        if ev[0] == 'O' and ev[2] == CHUNKS - 1:
                            start_all(gu_cp[v_col // LANES:k_col // LANES] + wd_cp)
        return 0
    lax.fori_loop(0, steps, lambda k, _: run('T', step_t, k), 0)
    lax.fori_loop(0, SUBS * CHUNKS, lambda k, _: run('M', step_m, k), 0)

    if last:
        for r in range(CHUNKS):
            for kind in ('G0', 'G1', 'G2'):
                remote(kind, 1, r).wait_send()
            out_copy(r).wait()
        return

    own_cp = pltpu.make_async_copy(own, own_out, osem.at[0])
    own_cp.start()
    n = CHUNKS * eighth
    mine = pl.ds(al(eig_own), eighth)
    def a():
        return r2[...].reshape(n, width)

    for cp in dkv_cp:
        cp.wait()
    kv = lax.dot_general(a(), wod[0:lat, :], NT, preferred_element_type=F32)
    inv = lax.rsqrt(jnp.mean(kv * kv, axis=-1, keepdims=True) + NORM_EPS)
    buf[:, mine, dq:dq + lat] = (kv * inv * kv_gain_ref[...].astype(F32)).astype(BF).reshape(CHUNKS, eighth, lat)
    kp = lax.dot_general(a(), wod[lat:lat + LANES, :], NT, preferred_element_type=F32)
    rope = dkv - lat
    lane = lax.broadcasted_iota(jnp.int32, (n, LANES), 1)
    swap = jnp.where(lane < rope // 2, pltpu.roll(kp, LANES - rope // 2, 1), pltpu.roll(kp, rope // 2, 1))
    kp = jnp.where(lane < rope, kp * cos_v[...].reshape(n, LANES) + swap * sin_v[...].reshape(n, LANES), 0.0)
    buf[:, mine, dq + lat:dq + lat + LANES] = kp.astype(BF).reshape(CHUNKS, eighth, LANES)
    for cp in dq_cp:
        cp.wait()
    total_sq = jnp.zeros((n, 1), F32)
    for j in range(dq // 512):
        v = jnp.dot(a(), wgu[:, j * 512:(j + 1) * 512], preferred_element_type=F32)
        total_sq = total_sq + jnp.sum(v * v, axis=-1, keepdims=True)
        for b in range(4):
            ctx[b, j * n:(j + 1) * n, :] = v[:, b * LANES:(b + 1) * LANES]
    inv = lax.rsqrt(total_sq * (1.0 / dq) + NORM_EPS)
    for j in range(dq // LANES):
        cs = slice(j * LANES, (j + 1) * LANES)
        v = ctx[j % 4, j // 4 * n:(j // 4 + 1) * n, :]
        buf[:, mine, cs] = (v * inv * q_gain_ref[:, cs].astype(F32)).astype(BF).reshape(CHUNKS, eighth, LANES)

    used = dq + lat + LANES
    first = dq // LANES * LANES

    def gather(k, off, rows_n, dev, lo=0):
        part = buf.at[:, pl.ds(al(off), rows_n), pl.ds(lo, used - lo)]
        cp = pltpu.make_async_remote_copy(src_ref=part, dst_ref=part, send_sem=ss.at[k, 0], recv_sem=rs.at[k, 0],
                                          device_id={'tp': dev}, device_id_type=MESH)
        cp.start()
        return cp

    for r in range(CHUNKS):
        granted('S2', 1, r)
    g0 = gather(9, eig_own, eighth, n2)
    g0.wait_recv()
    for r in range(CHUNKS):
        granted('S1', 1, r)
    g1 = gather(10, quart_own, quart, n1)
    g1.wait_recv()
    for r in range(CHUNKS):
        granted('S0', 1, r)
    g2 = gather(11, half_own, half, pair, first)
    outs = [pltpu.make_async_copy(buf.at[:, pl.ds(al(half_own), half), pl.ds(0, dq)], cq_out, osem.at[1]),
            pltpu.make_async_copy(buf.at[:, :, pl.ds(dq, lat)], ckv_out, osem.at[2]),
            pltpu.make_async_copy(buf.at[:, :, pl.ds(dq + lat, LANES)], kpe_out, osem.at[3])]
    outs[0].start()
    g2.wait_recv()
    start_all(outs[1:])
    for cp in (g0, g1, g2):
        cp.wait_send()
    own_cp.wait()
    for cp in outs:
        cp.wait()


def q_body(cq_ref, w_ref, uk_ref, cos_ref, sin_ref, lat_ref, rope_ref):
    group, qk = w_ref.shape[0], w_ref.shape[1]
    nope = uk_ref.shape[1] // group
    steps = lat_ref.shape[0]
    half = (qk - nope) // 2
    for g in range(group):
        w = jnp.concatenate([w_ref[g], w_ref[g, nope + half:, :], w_ref[g, nope:nope + half, :]], axis=0)
        q = lax.dot_general(cq_ref[...], w, NT, preferred_element_type=F32)
        rp, swap = q[:, nope:qk], q[:, qk:]
        rope = (rp * cos_ref[:, :2 * half] + swap * sin_ref[:, :2 * half]).astype(BF)
        lat = lax.dot_general(q[:, :nope].astype(BF), uk_ref[:, g * nope:(g + 1) * nope], NT, preferred_element_type=F32).astype(BF)
        lat_ref[:, g] = lat.reshape(steps, STEP, lat.shape[1])
        rope_ref[:, g, :, :2 * half] = rope.reshape(steps, STEP, 2 * half)
        rope_ref[:, g, :, 2 * half:] = jnp.zeros((steps, STEP, rope_ref.shape[3] - 2 * half), BF)


def q_heads(layer, c_q, w_uq_t, w_uk, cos_t, sin_t, group=2):
    n, rank = c_q.shape
    heads, qk = w_uq_t.shape[1], w_uq_t.shape[2]
    lat = w_uk.shape[1]
    nope = w_uk.shape[2] // heads
    steps = n // STEP
    q_lat, q_rope = pl.pallas_call(
        q_body, grid=(heads // group,),
        in_specs=[pl.BlockSpec((n, rank), lambda h: (0, 0)), pl.BlockSpec((None, group, qk, rank), lambda h: (layer, h, 0, 0)),
                  pl.BlockSpec((None, lat, group * nope), lambda h: (layer, 0, h)),
                  pl.BlockSpec((n, LANES), lambda h: (0, 0)), pl.BlockSpec((n, LANES), lambda h: (0, 0))],
        out_specs=[pl.BlockSpec((steps, group, STEP, lat), lambda h: (0, h, 0, 0)), pl.BlockSpec((steps, group, STEP, LANES), lambda h: (0, h, 0, 0))],
        out_shape=[jax.ShapeDtypeStruct((steps, heads, STEP, lat), BF), jax.ShapeDtypeStruct((steps, heads, STEP, LANES), BF)],
        name='q_heads', compiler_params=pltpu.CompilerParams(dimension_semantics=('arbitrary',)),
        cost_estimate=pl.CostEstimate(flops=2 * n * heads * (rank * qk + nope * lat), bytes_accessed=2 * rank * qk * heads, transcendentals=0),
    )(c_q, w_uq_t, w_uk, cos_t, sin_t)
    return q_lat.reshape(steps, heads * STEP, lat), q_rope.reshape(steps, heads * STEP, LANES)


def fused_layer(layer, last, scale, pos, c_new, k_new, w_uv, q_parts, ckv, kpe_t, resid, mlp_gain, w_o, w_gate, w_up, w_down, more):
    n, width = 2 * c_new.shape[0], w_down.shape[2]
    lat = c_new.shape[1]
    keys = kpe_t.shape[2]
    rows = n // CHUNKS
    depth, cols = w_o.shape[1], w_down.shape[1]
    vm = pl.BlockSpec(memory_space=pltpu.VMEM)
    hb = pl.BlockSpec(memory_space=pl.ANY)
    args = [pos, c_new, k_new, *w_uv, *q_parts, ckv, kpe_t, resid, mlp_gain, w_o, w_gate, w_up, w_down]
    specs = [pl.BlockSpec(memory_space=pltpu.SMEM), vm, vm] + [hb] * 9 + [vm, hb, hb, hb, hb]
    scratch = [pltpu.VMEM((width, 2 * cols), BF), pltpu.VMEM((cols, width), BF), pltpu.VMEM((CHUNKS, rows, width), BF),
               pltpu.VMEM((2, rows // 2, width), BF), pltpu.VMEM((CHUNKS, rows // 4, width), BF),
               pltpu.VMEM((CHUNKS, rows // 8, width), BF), pltpu.VMEM((CHUNKS, rows // 8, width), BF),
               pltpu.VMEM((rows, cols), BF), pltpu.VMEM((STEP * 16, keys), F32), pltpu.VMEM((lat // LANES, STEP * 16, LANES), F32),
               pltpu.VMEM((STEP * 16, LANES), jnp.int32), pltpu.VMEM((STEP * 16, LANES), F32), pltpu.VMEM((STEP * 16, LANES), F32)]
    if last:
        outs = jax.ShapeDtypeStruct((CHUNKS, rows, width), BF)
        out_specs = hb
    else:
        next_gain, q_gain, kv_gain, cos_t, sin_t, w_dq, w_dkv_t = more
        args += [next_gain, q_gain, kv_gain, cos_t, sin_t, w_dq, w_dkv_t]
        specs += [vm, vm, vm, hb, hb, hb, hb]
        outs = (jax.ShapeDtypeStruct((CHUNKS, rows // 8, width), BF), jax.ShapeDtypeStruct((CHUNKS, rows // 2, w_dq.shape[2]), BF),
                jax.ShapeDtypeStruct((CHUNKS, rows, kv_gain.shape[1]), BF), jax.ShapeDtypeStruct((CHUNKS, rows, LANES), BF))
        out_specs = (hb,) * 4
    scratch += [pltpu.SemaphoreType.DMA((width // WIDE,)), pltpu.SemaphoreType.DMA((2 * cols // LANES,)),
                pltpu.SemaphoreType.DMA((3,)), pltpu.SemaphoreType.DMA((4,)),
                pltpu.SemaphoreType.DMA((12, CHUNKS)), pltpu.SemaphoreType.DMA((12, CHUNKS)),
                pltpu.SemaphoreType.REGULAR((6, CHUNKS)), pltpu.SemaphoreType.REGULAR, pltpu.SemaphoreType.DMA((SLOTS,)), pltpu.SemaphoreType.DMA((SLOTS,)),
                pltpu.SemaphoreType.DMA((n // 2 // STEP, 4)), pltpu.SemaphoreType.DMA((4,)), pltpu.SemaphoreType.DMA((2, CHUNKS)), pltpu.SemaphoreType.DMA((2, CHUNKS))]
    if not last:
        scratch += [pltpu.VMEM((CHUNKS, rows // 8, LANES), F32)] * 2
    return pl.pallas_call(
        functools.partial(layer_body, layer, last, scale), in_specs=specs, out_specs=out_specs, out_shape=outs, scratch_shapes=scratch,
        name='layer_last' if last else 'layer_mid',
        compiler_params=pltpu.CompilerParams(collective_id=1 if last else 0, has_side_effects=True, vmem_limit_bytes=67043328),
        cost_estimate=pl.CostEstimate(flops=2 * n * (width * (depth + 3 * cols) + 8 * keys * 2 * lat), bytes_accessed=2 * width * (depth + 3 * cols) + 2 * n * keys * lat, transcendentals=n * cols),
    )(*args)


def solution(mesh):
    cache_spec = P(None, 'dp', None, None)
    head_spec = P(None, None, 'tp', None)
    weight_specs = (P(), P(), P(), P(), P(), head_spec, head_spec, head_spec, P(None, 'tp', None, None), P(), P(None, None, 'tp'), P(None, None, 'tp'), P(None, 'tp', None))
    in_specs = (P('dp', None), P('dp'), cache_spec, cache_spec) + weight_specs
    out_specs = (P('dp', None), P(None, 'dp', None), P(None, 'dp', None))

    def device_body(x_in, pos_ids, ckv_cache, kpe_cache, attn_gain, w_dq, q_gain, w_dkv, kv_gain, w_uq, w_uk, w_uv, w_o, mlp_gain, w_gate, w_up, w_down):
        n, width = x_in.shape
        rows = n // CHUNKS
        lat = w_uk.shape[1]
        nope = w_uk.shape[3]
        rope = kpe_cache.shape[3]
        half = rope // 2
        inv_freq = jnp.exp(jnp.arange(half, dtype=F32) * (-2.0 * math.log(ROPE_BASE) / rope))
        angles = pos_ids.astype(F32)[:, None] * inv_freq
        cos_p, sin_p = jnp.cos(angles), jnp.sin(angles)
        pad = jnp.zeros((n, LANES - rope), F32)
        cos_t = jnp.concatenate([cos_p, cos_p, pad], axis=1).reshape(CHUNKS, rows, LANES)
        sin_t = jnp.concatenate([-sin_p, sin_p, pad], axis=1).reshape(CHUNKS, rows, LANES)
        kpe_t = jnp.swapaxes(kpe_cache, 2, 3)
        w_dkv_t = jnp.swapaxes(w_dkv, 1, 2)
        w_o2 = w_o.reshape(w_o.shape[0], -1, width)
        scale = w_uq.shape[-1] ** -0.5

        ckv_2d = ckv_cache.reshape(ckv_cache.shape[0], -1, lat)
        kpe_2d = kpe_t.reshape(kpe_t.shape[0], -1, kpe_t.shape[3])
        core = lax.rem(lax.axis_index('tp'), 2)
        swap = [(i, i + 1 - 2 * (i % 2)) for i in range(mesh.shape['tp'])]

        def mine(v):
            v = v.reshape((CHUNKS, 2, rows // 2) + v.shape[1:])
            v = lax.dynamic_index_in_dim(v, core, 1, keepdims=False)
            return v.reshape((n // 2,) + v.shape[2:])

        def whole(v):
            other = lax.ppermute(v, 'tp', swap)
            lo = jnp.where(core == 0, v, other).reshape((CHUNKS, 1, rows // 2) + v.shape[1:])
            hi = jnp.where(core == 0, other, v).reshape((CHUNKS, 1, rows // 2) + v.shape[1:])
            return jnp.concatenate([lo, hi], axis=1).reshape((n,) + v.shape[1:])

        uq = [jnp.transpose(w_uq, (0, 2, 3, 1))]
        uk = [w_uk.reshape(w_uk.shape[0], lat, -1)]
        uv = [w_uv.reshape(w_uv.shape[0], lat, -1)]
        for w in (uq, uk, uv):
            w.append(lax.ppermute(w[0], 'tp', swap))
        pos_own = mine(pos_ids)
        cos_own, sin_own = mine(cos_t.reshape(n, LANES)), mine(sin_t.reshape(n, LANES))

        def q_parts(layer, c_q):
            (lat_a, rope_a), (lat_b, rope_b) = [q_heads(layer, c_q, uq[i], uk[i], cos_own, sin_own) for i in range(2)]
            return lat_a, lat_b, rope_a, rope_b

        normed = rms_norm(mine(x_in), attn_gain[0])
        c_q = rms_norm(jnp.dot(normed, w_dq[0], preferred_element_type=F32), q_gain[0])
        kv = jnp.dot(normed, w_dkv[0], preferred_element_type=F32)
        c_new0 = rms_norm(kv[:, :lat], kv_gain[0])
        k_new0 = rotate(kv[:, lat:], cos_own[:, :half], sin_own[:, half:rope]).astype(BF)
        k_pad0 = jnp.pad(k_new0, ((0, 0), (0, LANES - rope)))
        x_own, c_q, c_new1, k_pad1 = fused_layer(
            0, False, scale, pos_own, c_new0, k_pad0, uv, q_parts(0, c_q), ckv_2d, kpe_2d, x_in.reshape(CHUNKS, rows, width), mlp_gain[0:1], w_o2, w_gate, w_up, w_down,
            (attn_gain[1:2], q_gain[1:2], kv_gain[1:2], cos_t, sin_t, w_dq, w_dkv_t))
        c_new1 = c_new1.reshape(n, lat)
        k_pad1 = k_pad1.reshape(n, LANES)
        k_new1 = k_pad1[:, :rope]
        c_new0, k_new0 = whole(c_new0), whole(k_new0)
        x_out = fused_layer(1, True, scale, pos_own, mine(c_new1), mine(k_pad1), uv, q_parts(1, c_q.reshape(n // 2, -1)), ckv_2d, kpe_2d, x_own, mlp_gain[1:2], w_o2, w_gate, w_up, w_down, None)
        return x_out.reshape(n, width), jnp.stack([c_new0, c_new1]), jnp.stack([k_new0, k_new1])

    return jax.shard_map(device_body, mesh=mesh, in_specs=in_specs, out_specs=out_specs, check_vma=False)
```

```python
import functools
import math
import jax
import jax.numpy as jnp
from jax import lax
from jax.experimental import pallas as pl
from jax.experimental.pallas import tpu as pltpu
from jax.sharding import PartitionSpec as P

NORM_EPS = 1e-6
ROPE_BASE = 10000.0
BF = jnp.bfloat16
F32 = jnp.float32
NT = (((1,), (1,)), ((), ()))
MESH = pl.DeviceIdType.MESH

SUB = 8
LANES = 128
STEP = 16
SUBS = 5
SLOTS = 9
CHUNKS = 4
WIDE = 1024

ORDER_LAST = (
    'T', 'T', 'T', 'T', 'E00', 'T', 'T', 'O00', 'T', 'T', 'A000', 'E01', 'T', 'T',
    'O01', 'T', 'A100', 'T', 'A001', 'E02', 'T', 'A200', 'O02', 'T', 'A101', 'T', 'B000', 'A002',
    'T', 'E03', 'A201', 'O03', 'B100', 'B001', 'A003', 'B200', 'M', 'A102', 'M', 'M', 'B101', 'M',
    'A202', 'M', 'B201', 'M', 'A103', 'M', 'B002', 'A010', 'M', 'M', 'A203', 'M', 'B102', 'A011',
    'B003', 'B202', 'M', 'A110', 'M', 'M', 'M', 'A210', 'A111', 'M', 'B103', 'A012', 'B010', 'B203',
    'M', 'A211', 'M', 'M', 'A112', 'M', 'B011', 'M', 'B110', 'A212', 'A013', 'B210', 'B111', 'B012',
    'B211', 'A113', 'B112', 'A213', 'B212', 'B013', 'B113', 'B213',
)
ORDER_MID = (
    'T', 'T', 'T', 'T', 'E00', 'T', 'O00', 'T', 'T', 'A000', 'T', 'E01', 'T', 'O01',
    'T', 'A100', 'T', 'A001', 'T', 'E02', 'T', 'A200', 'O02', 'T', 'A101', 'T', 'B000', 'A002',
    'T', 'E03', 'A201', 'O03', 'B100', 'A003', 'B001', 'B200', 'M', 'M', 'A102', 'M', 'M', 'M',
    'A103', 'A202', 'A010', 'B101', 'A203', 'B201', 'M', 'M', 'B002', 'A110', 'M', 'M', 'B003', 'M',
    'A210', 'B102', 'A011', 'B202', 'M', 'M', 'B103', 'M', 'M', 'B203', 'M', 'A111', 'M', 'M',
    'A012', 'M', 'A211', 'M', 'M', 'A112', 'A013', 'A212', 'A113', 'A213',
)


def rms_norm(values, norm_gain):
    values = values.astype(F32)
    inv_rms = lax.rsqrt(jnp.mean(values * values, axis=-1, keepdims=True) + NORM_EPS)
    return (values * inv_rms * norm_gain.astype(F32)).astype(BF)


def rotate(values, cos_part, sin_part):
    half_dim = values.shape[-1] // 2
    lo_half = values[..., :half_dim]
    hi_half = values[..., half_dim:]
    return jnp.concatenate([lo_half * cos_part - hi_half * sin_part, hi_half * cos_part + lo_half * sin_part], axis=-1)


def layer_body(layer, last, scale, *refs):
    (pos_ref, cn_ref, kn_ref, uva_hbm, uvb_hbm, qa_hbm, qb_hbm, ra_hbm, rb_hbm, ckv_hbm, kpe_hbm, x_hbm, gain_ref, wo_hbm, wg_hbm, wu_hbm, wd_hbm), refs = refs[:17], refs[17:]
    if last:
        out_hbm, refs = refs[0], refs[1:]
    else:
        (next_gain_ref, q_gain_ref, kv_gain_ref, cos_hbm, sin_hbm, wdq_hbm, wdkv_hbm, own_out, cq_out, ckv_out, kpe_out), refs = refs[:11], refs[11:]
    (wgu, wod, buf, r0, r1, r2, own, act, sc, ctx, posv, rope_t, fresh_v, wsem, gsem, xsem, osem, ss, rs, ack, credit, csem, ksem, qsem, uvsem, es, er), refs = refs[:27], refs[27:]
    if not last:
        cos_v, sin_v = refs
    heads = 16
    own_heads = 8
    keys = sc.shape[1]
    n_lat = qa_hbm.shape[2]
    n_rope = kpe_hbm.shape[1] // (ckv_hbm.shape[1] // keys)
    steps = qa_hbm.shape[0]
    per = steps // CHUNKS
    total = steps * (STEP // SUB)
    blk = STEP * own_heads
    q_base = 3 * SUB * keys
    k_col = 4 * n_lat
    v_col = 3 * n_lat
    c_row = 4 * n_lat
    c_rows = STEP * per
    send_row = c_row + heads * c_rows
    ho_row = send_row + 2 * CHUNKS * c_rows
    depth = wo_hbm.shape[1]
    cols = wd_hbm.shape[1]
    width = wd_hbm.shape[2]
    rows = buf.shape[1]
    half, quart, eighth = rows // 2, rows // 4, rows // 8
    tiles = width // WIDE

    me = lax.axis_index('tp')
    c = lax.rem(me, 2)
    x = lax.rem(me // 2, 2)
    y = me // 4
    f = x * (1 - c) + y * c
    s = y * (1 - c) + x * c
    pair = y * 4 + x * 2 + (1 - c)
    n1 = (y * (1 - c) + (1 - y) * c) * 4 + ((1 - x) * (1 - c) + x * c) * 2 + c
    n2 = ((1 - y) * (1 - c) + y * c) * 4 + (x * (1 - c) + (1 - x) * c) * 2 + c
    half_own, half_oth = c * half, (1 - c) * half
    quart_own, quart_oth = half_own + f * quart, half_own + (1 - f) * quart
    eig_own, eig_oth = quart_own + s * eighth, quart_own + (1 - s) * eighth
    al = lambda v: pl.multiple_of(v, 16)

    barrier = pltpu.get_barrier_semaphore()
    for dev in (pair, n1, n2):
        pl.semaphore_signal(barrier, inc=1, device_id={'tp': dev}, device_id_type=MESH)

    def slot_at(slot):
        return pl.multiple_of(lax.rem(slot, 3) * (SUB * keys), SUB * keys), pl.multiple_of(slot // 3 * n_lat, n_lat)

    def cache_copies(t):
        slot = lax.rem(t, SLOTS)
        row, col = slot_at(slot)
        sub = STEP // SUB
        first = t // (per * sub) * rows + c * half + lax.rem(t, per * sub) * SUB
        return (pltpu.make_async_copy(ckv_hbm.at[layer, pl.ds(pl.multiple_of(first * keys, SUB * keys), SUB * keys)],
                                      wgu.at[pl.ds(row, SUB * keys), pl.ds(col, n_lat)], csem.at[slot]),
                pltpu.make_async_copy(kpe_hbm.at[layer, pl.ds(pl.multiple_of(first * n_rope, SUB * n_rope), SUB * n_rope)],
                                      wgu.at[pl.ds(pl.multiple_of(slot * (SUB * n_rope), SUB * n_rope), SUB * n_rope), pl.ds(k_col, keys)], ksem.at[slot]))

    def q_at(k):
        return pl.multiple_of(q_base + lax.rem(k, 4) * (STEP * heads), STEP * heads), pl.multiple_of(k // 4 * n_lat, n_lat)

    def q_copies(k):
        row, col = q_at(k)
        out = []
        for i, (lat_hbm, rope_hbm) in enumerate(((qa_hbm, ra_hbm), (qb_hbm, rb_hbm))):
            out.append(pltpu.make_async_copy(lat_hbm.at[k], wgu.at[pl.ds(row + i * blk, blk), pl.ds(col, n_lat)], qsem.at[k, 2 * i]))
            out.append(pltpu.make_async_copy(rope_hbm.at[k], wod.at[pl.ds(depth, LANES), pl.ds(pl.multiple_of((2 * k + i) * LANES, LANES), LANES)], qsem.at[k, 2 * i + 1]))
        return out

    uv_cp = []
    for i, uv_hbm in enumerate((uva_hbm, uvb_hbm)):
        for b in range(2):
            uv_cp.append(pltpu.make_async_copy(uv_hbm.at[layer, :, pl.ds(b * n_lat, n_lat)], wgu.at[pl.ds((2 * i + b) * n_lat, n_lat), pl.ds(v_col, n_lat)], uvsem.at[2 * i + b]))

    def start_all(cps):
        for cp in cps:
            cp.start()

    def wait_all(cps):
        for cp in cps:
            cp.wait()

    start_all(q_copies(0))
    for t in range(STEP // SUB):
        start_all(cache_copies(t))
    start_all(q_copies(1))
    for t in range(STEP // SUB, SLOTS):
        start_all(cache_copies(t))

    def more_q(k, _):
        start_all(q_copies(k))
        return 0
    lax.fori_loop(2, steps, more_q, 0)
    start_all(uv_cp)

    wo_cp = [pltpu.make_async_copy(wo_hbm.at[layer, :, pl.ds(j * WIDE, WIDE)], wod.at[pl.ds(0, depth), pl.ds(j * WIDE, WIDE)], wsem.at[j]) for j in range(tiles)]
    for cp in wo_cp:
        cp.start()
    if last:
        x_cp = [pltpu.make_async_copy(x_hbm, own, xsem.at[0])]
    else:
        x_cp = [pltpu.make_async_copy(x_hbm.at[:, pl.ds(al(eig_own), eighth)], own, xsem.at[0]),
                pltpu.make_async_copy(cos_hbm.at[:, pl.ds(al(eig_own), eighth)], cos_v, xsem.at[1]),
                pltpu.make_async_copy(sin_hbm.at[:, pl.ds(al(eig_own), eighth)], sin_v, xsem.at[2])]
    for cp in x_cp:
        cp.start()
    gu_cp = []
    for j in range(cols // LANES):
        gu_cp.append(pltpu.make_async_copy(wg_hbm.at[layer, :, pl.ds(j * LANES, LANES)], wgu.at[:, pl.ds(2 * j * LANES, LANES)], gsem.at[2 * j]))
        gu_cp.append(pltpu.make_async_copy(wu_hbm.at[layer, :, pl.ds(j * LANES, LANES)], wgu.at[:, pl.ds((2 * j + 1) * LANES, LANES)], gsem.at[2 * j + 1]))
    wd_cp = [pltpu.make_async_copy(wd_hbm.at[layer, :, pl.ds(j * WIDE, WIDE)], wod.at[:, pl.ds(j * WIDE, WIDE)], wsem.at[j]) for j in range(tiles)]
    if not last:
        dq = wdq_hbm.shape[2]
        dkv = wdkv_hbm.shape[1]
        lat = kv_gain_ref.shape[1]
        dq_cp = [pltpu.make_async_copy(wdq_hbm.at[layer + 1, :, pl.ds(j * 256, 256)], wgu.at[:, pl.ds(j * 256, 256)], gsem.at[j]) for j in range(dq // 256)]
        dkv_cp = [pltpu.make_async_copy(wdkv_hbm.at[layer + 1], wod.at[pl.ds(0, dkv)], wsem.at[0])]
    pl.semaphore_wait(barrier, 3)

    def remote(kind, ph, r):
        dev = {'0': pair, '1': n1, '2': n2}[kind[1]] if kind[0] == 'S' else {'0': n2, '1': n1, '2': pair}[kind[1]]
        k = 6 * ph + ('S0', 'S1', 'S2', 'G0', 'G1', 'G2').index(kind)
        if kind == 'S0':
            src, dst = buf.at[r, pl.ds(al(half_oth), half)], r0.at[r % 2]
        elif kind == 'S1':
            src, dst = buf.at[r, pl.ds(al(quart_oth), quart)], r1.at[r]
        elif kind == 'S2':
            src, dst = buf.at[r, pl.ds(al(eig_oth), eighth)], r2.at[r]
        else:
            off, n = {'G0': (eig_own, eighth), 'G1': (quart_own, quart), 'G2': (half_own, half)}[kind]
            src = buf.at[r, pl.ds(al(off), n)]
            dst = src
        return pltpu.make_async_remote_copy(src_ref=src, dst_ref=dst, send_sem=ss.at[k, r], recv_sem=rs.at[k, r],
                                            device_id={'tp': dev}, device_id_type=MESH)

    def send(kind, ph, r):
        if kind == 'S0' and (ph, r) not in ((0, 0), (0, 1)):
            pl.semaphore_wait(credit, 1)
        remote(kind, ph, r).start()

    def landed(kind, ph, r, dev):
        remote(kind, ph, r).wait_recv()
        remote(kind, ph, r).wait_send()
        pl.semaphore_signal(ack.at[3 * ph + int(kind[1]), r], inc=1, device_id={'tp': dev}, device_id_type=MESH)

    def granted(kind, ph, r):
        pl.semaphore_wait(ack.at[3 * ph + int(kind[1]), r], 1)

    def add_rows(r, off, src, src_off, n, slot):
        def tile(t, _):
            cs = pl.ds(pl.multiple_of(t * WIDE, WIDE), WIDE)
            rw = pl.ds(al(off), n)
            buf[r, rw, cs] = (buf[r, rw, cs].astype(F32) + src[slot, pl.ds(al(src_off), n), cs].astype(F32)).astype(BF)
            return 0
        lax.fori_loop(0, tiles, tile, 0)

    def out_copy(r):
        return pltpu.make_async_copy(buf.at[r], out_hbm.at[r], osem.at[r])

    def pair_copy(r, q):
        src = wgu.at[pl.ds(send_row + (2 * r + q) * c_rows, c_rows), pl.ds(v_col, n_lat)]
        dst = wgu.at[pl.ds(al(ho_row + (2 * r + q) * rows + c * c_rows), c_rows), pl.ds(v_col, n_lat)]
        return pltpu.make_async_remote_copy(src_ref=src, dst_ref=dst, send_sem=es.at[q, r], recv_sem=er.at[q, r],
                                            device_id={'tp': pair}, device_id_type=MESH)

    def step_e(r):
        if r == 0:
            wait_all(uv_cp)
        for own_side in (False, True):
            for h in range(own_heads):
                g = h if own_side else h + own_heads
                val = jnp.dot(wgu[c_row + g * c_rows:c_row + (g + 1) * c_rows, v_col:v_col + n_lat],
                              wgu[g // 4 * n_lat:(g // 4 + 1) * n_lat, v_col + g % 4 * LANES:v_col + (g % 4 + 1) * LANES], preferred_element_type=F32).astype(BF)
                cs = slice(v_col + h % 4 * LANES, v_col + (h % 4 + 1) * LANES)
                if own_side:
                    wgu[pl.ds(al(ho_row + (2 * r + h // 4) * rows + c * c_rows), c_rows), cs] = val
                else:
                    wgu[send_row + (2 * r + h // 4) * c_rows:send_row + (2 * r + h // 4 + 1) * c_rows, cs] = val
        for q in range(2):
            pair_copy(r, q).start()

    def step_o(r):
        for q in range(2):
            pair_copy(r, q).wait_recv()
            pair_copy(r, q).wait_send()
        if r == 0:
            for cp in x_cp:
                cp.wait()

        def tile(t, _):
            if r == 0:
                pltpu.make_async_copy(wo_hbm.at[layer, :, pl.ds(0, WIDE)], wod.at[pl.ds(0, depth), pl.ds(0, WIDE)], wsem.at[t]).wait()
            cs = pl.ds(pl.multiple_of(t * WIDE, WIDE), WIDE)
            acc = sum(jnp.dot(wgu[ho_row + (2 * r + q) * rows:ho_row + (2 * r + q + 1) * rows, v_col:v_col + n_lat], wod[q * n_lat:(q + 1) * n_lat, cs], preferred_element_type=F32) for q in range(2))
            buf[r, :, cs] = acc.astype(BF)
            return 0
        lax.fori_loop(0, tiles, tile, 0)
        send('S0', 0, r)

    def step_m(m):
        r = m // SUBS
        part = lax.rem(m, SUBS)
        n_gate = cols // LANES // 3

        def gate(j, _):
            @pl.when(r == 0)
            def _():
                for i in range(2):
                    pltpu.make_async_copy(wg_hbm.at[layer, :, pl.ds(0, LANES)], wgu.at[:, pl.ds(0, LANES)], gsem.at[2 * j + i]).wait()
            cs = pl.ds(pl.multiple_of(j * 256, 256), 256)
            pre = jnp.dot(buf[r], wgu[:, cs], preferred_element_type=F32)
            act[:, pl.ds(pl.multiple_of(j * LANES, LANES), LANES)] = (jax.nn.silu(pre[:, :LANES]) * pre[:, LANES:]).astype(BF)
            return 0

        def tile(t, _):
            cs = pl.ds(pl.multiple_of(t * WIDE, WIDE), WIDE)
            buf[r, :, cs] = jnp.dot(act[...], wod[:, cs], preferred_element_type=F32).astype(BF)
            return 0

        @pl.when(part < 3)
        def _():
            lax.fori_loop(part * n_gate, (part + 1) * n_gate, gate, 0)

        @pl.when(m == 3)
        def _():
            wait_all(wd_cp)

        @pl.when(part == 3)
        def _():
            for kind in ('G0', 'G1', 'G2'):
                remote(kind, 0, r).wait_send()

        @pl.when(part >= 3)
        def _():
            cut = (tiles + 1) // 2
            lax.fori_loop((part - 3) * cut, cut + (part - 3) * (tiles - cut), tile, 0)

    def reduce_own(ph, r):
        def tile(t, acc):
            cs = pl.ds(pl.multiple_of(t * WIDE, WIDE), WIDE)
            v = own[r, :, cs].astype(F32) + (buf[r, pl.ds(al(eig_own), eighth), cs].astype(F32) + r2[r, :, cs].astype(F32))
            v = v.astype(BF)
            own[r, :, cs] = v
            if ph == 1 and last:
                buf[r, pl.ds(al(eig_own), eighth), cs] = v
            v = v.astype(F32)
            return acc + v * v
        acc = lax.fori_loop(0, tiles, tile, jnp.zeros((eighth, WIDE), F32))
        return lax.rsqrt(jnp.sum(acc, axis=-1, keepdims=True) * (1.0 / width) + NORM_EPS)

    def norm_own(r, inv, gain, put):
        def tile(t, _):
            cs = pl.ds(pl.multiple_of(t * WIDE, WIDE), WIDE)
            put(r, cs, (own[r, :, cs].astype(F32) * inv * gain[:, cs].astype(F32)).astype(BF))
            return 0
        lax.fori_loop(0, tiles, tile, 0)

    def put_buf(r, cs, v):
        buf[r, pl.ds(al(eig_own), eighth), cs] = v

    def put_r2(r, cs, v):
        r2[r, :, cs] = v

    def step_t(k):
        rows_n = STEP * heads
        nsub = STEP // SUB
        wait_all(q_copies(k))
        q_row, q_col = q_at(k)
        blocks = [(slice(b * LANES, (b + 1) * LANES), pl.ds(pl.multiple_of(q_col + b * LANES, LANES), LANES)) for b in range(n_lat // LANES)]
        for b, (_, cs) in enumerate(blocks):
            ctx[b] = wgu[pl.ds(q_row, rows_n), cs].astype(F32)
        for i in range(2):
            rope_t[i * blk:(i + 1) * blk, :] = wod[depth:depth + LANES, pl.ds(pl.multiple_of((2 * k + i) * LANES, LANES), LANES)].astype(F32)
        cn = cn_ref[pl.ds(pl.multiple_of(k * STEP, STEP), STEP), :].astype(F32)
        kn = kn_ref[pl.ds(pl.multiple_of(k * STEP, STEP), STEP), :].astype(F32)
        slots = []
        for j in range(nsub):
            t = k * nsub + j
            wait_all(cache_copies(t))
            slot = lax.rem(t, SLOTS)
            row, col = slot_at(slot)
            slots.append((row, col))
            k_row = pl.multiple_of(slot * (SUB * n_rope), SUB * n_rope)
            for e in range(SUB):
                i = j * SUB + e
                q = jnp.concatenate([ctx[b, pl.ds(i, heads, stride=STEP), :] for b in range(n_lat // LANES)], axis=1)
                qr = rope_t[pl.ds(i, heads, stride=STEP), :]
                s_i = lax.dot_general(q.astype(BF), wgu[pl.ds(row + e * keys, keys), pl.ds(col, n_lat)], NT, preferred_element_type=F32)
                s_i = s_i + jnp.dot(qr[:, :n_rope].astype(BF), wgu[pl.ds(k_row + e * n_rope, n_rope), pl.ds(k_col, keys)], preferred_element_type=F32)
                sc[i * heads:(i + 1) * heads, :] = s_i
                part = qr * kn[i:i + 1]
                for b, (lo, _) in enumerate(blocks):
                    part = part + q[:, lo] * cn[i:i + 1, lo]
                fresh_v[i * heads:(i + 1) * heads, :] = part
                posv[i * heads:(i + 1) * heads, :] = jnp.full((heads, LANES), pos_ref[k * STEP + i], jnp.int32)
        col_id = lax.broadcasted_iota(jnp.int32, (rows_n, keys), 1)
        pv = posv[:, 0:1]
        fresh = jnp.sum(fresh_v[...], axis=-1, keepdims=True)
        hit = col_id == pv
        sco = jnp.where(hit, fresh, sc[...]) * scale
        sco = jnp.where(col_id <= pv, sco, -jnp.inf)
        e_x = jnp.exp(sco - jnp.max(sco, axis=-1, keepdims=True))
        w = (e_x / jnp.sum(e_x, axis=-1, keepdims=True)).astype(BF).astype(F32)
        fresh_v[...] = jnp.broadcast_to(jnp.sum(jnp.where(hit, w, 0.0), axis=-1, keepdims=True), fresh_v.shape)
        sc[...] = jnp.where(hit, 0.0, w)
        for j in range(nsub):
            row, col = slots[j]
            for e in range(SUB):
                i = j * SUB + e
                rw = slice(i * heads, (i + 1) * heads)
                val = jnp.dot(sc[rw, :].astype(BF), wgu[pl.ds(row + e * keys, keys), pl.ds(col, n_lat)], preferred_element_type=F32)
                for b, (lo, _) in enumerate(blocks):
                    ctx[b, rw, :] = val[:, lo] + fresh_v[rw, :] * cn[i:i + 1, lo]
            nxt = k * nsub + j + SLOTS

            @pl.when(nxt < total)
            def _():
                start_all(cache_copies(nxt))
        for h in range(heads):
            ctx_h = jnp.concatenate([ctx[b, pl.ds(h, STEP, stride=heads), :] for b in range(n_lat // LANES)], axis=1)
            wgu[pl.ds(al(c_row + h * c_rows + lax.rem(k, per) * STEP), STEP), v_col:v_col + n_lat] = ctx_h.astype(BF)

    def event(op, ph, r):
        if op == 'E':
            step_e(r)
        elif op == 'O':
            step_o(r)
        elif op == 'A0':
            landed('S0', ph, r, pair)
            add_rows(r, quart_oth, r0, (1 - f) * quart, quart, r % 2)
            add_rows(r, quart_own, r0, f * quart, quart, r % 2)
            if (ph, r) not in ((1, 2), (1, 3)):
                pl.semaphore_signal(credit, inc=1, device_id={'tp': pair}, device_id_type=MESH)
            send('S1', ph, r)
        elif op == 'A1':
            landed('S1', ph, r, n1)
            add_rows(r, eig_oth, r1, (1 - s) * eighth, eighth, r)
            add_rows(r, eig_own, r1, s * eighth, eighth, r)
            send('S2', ph, r)
        elif op == 'A2':
            landed('S2', ph, r, n2)
            inv = reduce_own(ph, r)
            if ph == 0:
                norm_own(r, inv, gain_ref, put_buf)
            elif not last:
                norm_own(r, inv, next_gain_ref, put_r2)
            if ph == 0 or last:
                granted('S2', ph, r)
                send('G0', ph, r)
        elif op == 'B0':
            remote('G0', ph, r).wait_recv()
            granted('S1', ph, r)
            send('G1', ph, r)
        elif op == 'B1':
            remote('G1', ph, r).wait_recv()
            granted('S0', ph, r)
            send('G2', ph, r)
        elif op == 'B2':
            remote('G2', ph, r).wait_recv()
            if ph == 1:
                out_copy(r).start()


    hooks = {'T': [[]], 'M': [[]]}
    now = 'T'
    for token in (ORDER_LAST if last else ORDER_MID):
        if token in hooks:
            now = token
            hooks[now].append([])
        else:
            hooks[now][-1].append((token[:-2], int(token[-2]), int(token[-1])))

    def run(name, step, k):
        step(k)
        for at, evs in enumerate(hooks[name][1:]):
            if evs or name == 'M':
                @pl.when(k == at)
                def _(at=at, evs=evs):
                    if name == 'M' and at % SUBS == SUBS - 1:
                        send('S0', 1, at // SUBS)
                        if at == SUBS * CHUNKS - 1 and not last:
                            start_all(dkv_cp)
                    if name == 'M' and at == SUBS * CHUNKS - 3 and not last:
                        start_all(dq_cp)
                    for ev in evs:
                        if ev[0] == 'O' and ev[2] == CHUNKS - 1:
                            start_all(gu_cp[:v_col // LANES] + gu_cp[k_col // LANES:])
                        event(*ev)
                        if ev[0] == 'O' and ev[2] == CHUNKS - 1:
                            start_all(gu_cp[v_col // LANES:k_col // LANES] + wd_cp)
        return 0
    lax.fori_loop(0, steps, lambda k, _: run('T', step_t, k), 0)
    lax.fori_loop(0, SUBS * CHUNKS, lambda k, _: run('M', step_m, k), 0)

    if last:
        for r in range(CHUNKS):
            for kind in ('G0', 'G1', 'G2'):
                remote(kind, 1, r).wait_send()
            out_copy(r).wait()
        return

    own_cp = pltpu.make_async_copy(own, own_out, osem.at[0])
    own_cp.start()
    n = CHUNKS * eighth
    mine = pl.ds(al(eig_own), eighth)
    def a():
        return r2[...].reshape(n, width)

    for cp in dkv_cp:
        cp.wait()
    kv = lax.dot_general(a(), wod[0:lat, :], NT, preferred_element_type=F32)
    inv = lax.rsqrt(jnp.mean(kv * kv, axis=-1, keepdims=True) + NORM_EPS)
    buf[:, mine, dq:dq + lat] = (kv * inv * kv_gain_ref[...].astype(F32)).astype(BF).reshape(CHUNKS, eighth, lat)
    kp = lax.dot_general(a(), wod[lat:lat + LANES, :], NT, preferred_element_type=F32)
    rope = dkv - lat
    lane = lax.broadcasted_iota(jnp.int32, (n, LANES), 1)
    swap = jnp.where(lane < rope // 2, pltpu.roll(kp, LANES - rope // 2, 1), pltpu.roll(kp, rope // 2, 1))
    kp = jnp.where(lane < rope, kp * cos_v[...].reshape(n, LANES) + swap * sin_v[...].reshape(n, LANES), 0.0)
    buf[:, mine, dq + lat:dq + lat + LANES] = kp.astype(BF).reshape(CHUNKS, eighth, LANES)
    for cp in dq_cp:
        cp.wait()
    total_sq = jnp.zeros((n, 1), F32)
    for j in range(dq // 512):
        v = jnp.dot(a(), wgu[:, j * 512:(j + 1) * 512], preferred_element_type=F32)
        total_sq = total_sq + jnp.sum(v * v, axis=-1, keepdims=True)
        for b in range(4):
            ctx[b, j * n:(j + 1) * n, :] = v[:, b * LANES:(b + 1) * LANES]
    inv = lax.rsqrt(total_sq * (1.0 / dq) + NORM_EPS)
    for j in range(dq // LANES):
        cs = slice(j * LANES, (j + 1) * LANES)
        v = ctx[j % 4, j // 4 * n:(j // 4 + 1) * n, :]
        buf[:, mine, cs] = (v * inv * q_gain_ref[:, cs].astype(F32)).astype(BF).reshape(CHUNKS, eighth, LANES)

    used = dq + lat + LANES
    first = dq // LANES * LANES

    def gather(k, off, rows_n, dev, lo=0):
        part = buf.at[:, pl.ds(al(off), rows_n), pl.ds(lo, used - lo)]
        cp = pltpu.make_async_remote_copy(src_ref=part, dst_ref=part, send_sem=ss.at[k, 0], recv_sem=rs.at[k, 0],
                                          device_id={'tp': dev}, device_id_type=MESH)
        cp.start()
        return cp

    for r in range(CHUNKS):
        granted('S2', 1, r)
    g0 = gather(9, eig_own, eighth, n2)
    g0.wait_recv()
    for r in range(CHUNKS):
        granted('S1', 1, r)
    g1 = gather(10, quart_own, quart, n1)
    g1.wait_recv()
    for r in range(CHUNKS):
        granted('S0', 1, r)
    g2 = gather(11, half_own, half, pair, first)
    outs = [pltpu.make_async_copy(buf.at[:, pl.ds(al(half_own), half), pl.ds(0, dq)], cq_out, osem.at[1]),
            pltpu.make_async_copy(buf.at[:, :, pl.ds(dq, lat)], ckv_out, osem.at[2]),
            pltpu.make_async_copy(buf.at[:, :, pl.ds(dq + lat, LANES)], kpe_out, osem.at[3])]
    outs[0].start()
    g2.wait_recv()
    start_all(outs[1:])
    for cp in (g0, g1, g2):
        cp.wait_send()
    own_cp.wait()
    for cp in outs:
        cp.wait()


def q_body(layer, cq_ref, w_hbm, uk_ref, cos_ref, sin_ref, lat_hbm, rope_hbm, wv, latv, ropev, wsem, lsem, rsem):
    heads, qk = wv.shape[:2]
    nope = uk_ref.shape[1] // heads
    steps = latv.shape[1]
    half = (qk - nope) // 2

    def load(h):
        return pltpu.make_async_copy(w_hbm.at[layer, h], wv.at[h], wsem.at[h])

    def stores(h):
        return (pltpu.make_async_copy(latv.at[h], lat_hbm.at[:, h], lsem.at[h]), pltpu.make_async_copy(ropev.at[h], rope_hbm.at[:, h], rsem.at[h]))

    for h in range(heads):
        load(h).start()
    ropev[...] = jnp.zeros_like(ropev)

    def head(h, _):
        load(h).wait()
        w = jnp.concatenate([wv[h], wv[h, nope + half:, :], wv[h, nope:nope + half, :]], axis=0)
        q = lax.dot_general(cq_ref[...], w, NT, preferred_element_type=F32)
        rp, swap = q[:, nope:qk], q[:, qk:]
        rope = (rp * cos_ref[:, :2 * half] + swap * sin_ref[:, :2 * half]).astype(BF)
        uk = uk_ref[:, pl.ds(pl.multiple_of(h * nope, nope), nope)]
        lat = lax.dot_general(q[:, :nope].astype(BF), uk, NT, preferred_element_type=F32).astype(BF)
        latv[h] = lat.reshape(steps, STEP, lat.shape[1])
        ropev[h, :, :, :2 * half] = rope.reshape(steps, STEP, 2 * half)
        for cp in stores(h):
            cp.start()
        return 0
    lax.fori_loop(0, heads, head, 0)
    for h in range(heads):
        for cp in stores(h):
            cp.wait()


def q_heads(layer, c_q, w_uq_t, w_uk, cos_t, sin_t):
    n, rank = c_q.shape
    heads, qk = w_uq_t.shape[1], w_uq_t.shape[2]
    lat = w_uk.shape[1]
    nope = w_uk.shape[2] // heads
    steps = n // STEP
    hb = pl.BlockSpec(memory_space=pl.ANY)
    q_lat, q_rope = pl.pallas_call(
        functools.partial(q_body, layer), grid=(1,),
        in_specs=[pl.BlockSpec((n, rank), lambda i: (0, 0)), hb, pl.BlockSpec((None, lat, heads * nope), lambda i: (layer, 0, 0)),
                  pl.BlockSpec((n, LANES), lambda i: (0, 0)), pl.BlockSpec((n, LANES), lambda i: (0, 0))],
        out_specs=[hb, hb],
        out_shape=[jax.ShapeDtypeStruct((steps, heads, STEP, lat), BF), jax.ShapeDtypeStruct((steps, heads, STEP, LANES), BF)],
        scratch_shapes=[pltpu.VMEM((heads, qk, rank), BF), pltpu.VMEM((heads, steps, STEP, lat), BF), pltpu.VMEM((heads, steps, STEP, LANES), BF)]
        + [pltpu.SemaphoreType.DMA((heads,))] * 3,
        name='q_heads',
        cost_estimate=pl.CostEstimate(flops=2 * n * heads * (rank * qk + nope * lat), bytes_accessed=2 * rank * qk * heads, transcendentals=0),
    )(c_q, w_uq_t, w_uk, cos_t, sin_t)
    return q_lat.reshape(steps, heads * STEP, lat), q_rope.reshape(steps, heads * STEP, LANES)


def fused_layer(layer, last, scale, pos, c_new, k_new, w_uv, q_parts, ckv, kpe_t, resid, mlp_gain, w_o, w_gate, w_up, w_down, more):
    n, width = 2 * c_new.shape[0], w_down.shape[2]
    lat = c_new.shape[1]
    keys = kpe_t.shape[2]
    rows = n // CHUNKS
    depth, cols = w_o.shape[1], w_down.shape[1]
    vm = pl.BlockSpec(memory_space=pltpu.VMEM)
    hb = pl.BlockSpec(memory_space=pl.ANY)
    args = [pos, c_new, k_new, *w_uv, *q_parts, ckv, kpe_t, resid, mlp_gain, w_o, w_gate, w_up, w_down]
    specs = [pl.BlockSpec(memory_space=pltpu.SMEM), vm, vm] + [hb] * 9 + [vm, hb, hb, hb, hb]
    scratch = [pltpu.VMEM((width, 2 * cols), BF), pltpu.VMEM((cols, width), BF), pltpu.VMEM((CHUNKS, rows, width), BF),
               pltpu.VMEM((2, rows // 2, width), BF), pltpu.VMEM((CHUNKS, rows // 4, width), BF),
               pltpu.VMEM((CHUNKS, rows // 8, width), BF), pltpu.VMEM((CHUNKS, rows // 8, width), BF),
               pltpu.VMEM((rows, cols), BF), pltpu.VMEM((STEP * 16, keys), F32), pltpu.VMEM((lat // LANES, STEP * 16, LANES), F32),
               pltpu.VMEM((STEP * 16, LANES), jnp.int32), pltpu.VMEM((STEP * 16, LANES), F32), pltpu.VMEM((STEP * 16, LANES), F32)]
    if last:
        outs = jax.ShapeDtypeStruct((CHUNKS, rows, width), BF)
        out_specs = hb
    else:
        next_gain, q_gain, kv_gain, cos_t, sin_t, w_dq, w_dkv_t = more
        args += [next_gain, q_gain, kv_gain, cos_t, sin_t, w_dq, w_dkv_t]
        specs += [vm, vm, vm, hb, hb, hb, hb]
        outs = (jax.ShapeDtypeStruct((CHUNKS, rows // 8, width), BF), jax.ShapeDtypeStruct((CHUNKS, rows // 2, w_dq.shape[2]), BF),
                jax.ShapeDtypeStruct((CHUNKS, rows, kv_gain.shape[1]), BF), jax.ShapeDtypeStruct((CHUNKS, rows, LANES), BF))
        out_specs = (hb,) * 4
    scratch += [pltpu.SemaphoreType.DMA((width // WIDE,)), pltpu.SemaphoreType.DMA((2 * cols // LANES,)),
                pltpu.SemaphoreType.DMA((3,)), pltpu.SemaphoreType.DMA((4,)),
                pltpu.SemaphoreType.DMA((12, CHUNKS)), pltpu.SemaphoreType.DMA((12, CHUNKS)),
                pltpu.SemaphoreType.REGULAR((6, CHUNKS)), pltpu.SemaphoreType.REGULAR, pltpu.SemaphoreType.DMA((SLOTS,)), pltpu.SemaphoreType.DMA((SLOTS,)),
                pltpu.SemaphoreType.DMA((n // 2 // STEP, 4)), pltpu.SemaphoreType.DMA((4,)), pltpu.SemaphoreType.DMA((2, CHUNKS)), pltpu.SemaphoreType.DMA((2, CHUNKS))]
    if not last:
        scratch += [pltpu.VMEM((CHUNKS, rows // 8, LANES), F32)] * 2
    return pl.pallas_call(
        functools.partial(layer_body, layer, last, scale), in_specs=specs, out_specs=out_specs, out_shape=outs, scratch_shapes=scratch,
        name='layer_last' if last else 'layer_mid',
        compiler_params=pltpu.CompilerParams(collective_id=1 if last else 0, has_side_effects=True, vmem_limit_bytes=67043328),
        cost_estimate=pl.CostEstimate(flops=2 * n * (width * (depth + 3 * cols) + 8 * keys * 2 * lat), bytes_accessed=2 * width * (depth + 3 * cols) + 2 * n * keys * lat, transcendentals=n * cols),
    )(*args)


def solution(mesh):
    cache_spec = P(None, 'dp', None, None)
    head_spec = P(None, None, 'tp', None)
    weight_specs = (P(), P(), P(), P(), P(), head_spec, head_spec, head_spec, P(None, 'tp', None, None), P(), P(None, None, 'tp'), P(None, None, 'tp'), P(None, 'tp', None))
    in_specs = (P('dp', None), P('dp'), cache_spec, cache_spec) + weight_specs
    out_specs = (P('dp', None), P(None, 'dp', None), P(None, 'dp', None))

    def device_body(x_in, pos_ids, ckv_cache, kpe_cache, attn_gain, w_dq, q_gain, w_dkv, kv_gain, w_uq, w_uk, w_uv, w_o, mlp_gain, w_gate, w_up, w_down):
        n, width = x_in.shape
        rows = n // CHUNKS
        lat = w_uk.shape[1]
        nope = w_uk.shape[3]
        rope = kpe_cache.shape[3]
        half = rope // 2
        inv_freq = jnp.exp(jnp.arange(half, dtype=F32) * (-2.0 * math.log(ROPE_BASE) / rope))
        angles = pos_ids.astype(F32)[:, None] * inv_freq
        cos_p, sin_p = jnp.cos(angles), jnp.sin(angles)
        pad = jnp.zeros((n, LANES - rope), F32)
        cos_t = jnp.concatenate([cos_p, cos_p, pad], axis=1).reshape(CHUNKS, rows, LANES)
        sin_t = jnp.concatenate([-sin_p, sin_p, pad], axis=1).reshape(CHUNKS, rows, LANES)
        kpe_t = jnp.swapaxes(kpe_cache, 2, 3)
        w_dkv_t = jnp.swapaxes(w_dkv, 1, 2)
        w_o2 = w_o.reshape(w_o.shape[0], -1, width)
        scale = w_uq.shape[-1] ** -0.5

        ckv_2d = ckv_cache.reshape(ckv_cache.shape[0], -1, lat)
        kpe_2d = kpe_t.reshape(kpe_t.shape[0], -1, kpe_t.shape[3])
        core = lax.rem(lax.axis_index('tp'), 2)
        swap = [(i, i + 1 - 2 * (i % 2)) for i in range(mesh.shape['tp'])]

        def mine(v):
            v = v.reshape((CHUNKS, 2, rows // 2) + v.shape[1:])
            v = lax.dynamic_index_in_dim(v, core, 1, keepdims=False)
            return v.reshape((n // 2,) + v.shape[2:])

        def whole(v):
            other = lax.ppermute(v, 'tp', swap)
            lo = jnp.where(core == 0, v, other).reshape((CHUNKS, 1, rows // 2) + v.shape[1:])
            hi = jnp.where(core == 0, other, v).reshape((CHUNKS, 1, rows // 2) + v.shape[1:])
            return jnp.concatenate([lo, hi], axis=1).reshape((n,) + v.shape[1:])

        uq = [jnp.transpose(w_uq, (0, 2, 3, 1))]
        uk = [w_uk.reshape(w_uk.shape[0], lat, -1)]
        uv = [w_uv.reshape(w_uv.shape[0], lat, -1)]
        for w in (uq, uk, uv):
            w.append(lax.ppermute(w[0], 'tp', swap))
        pos_own = mine(pos_ids)
        cos_own, sin_own = mine(cos_t.reshape(n, LANES)), mine(sin_t.reshape(n, LANES))

        def q_parts(layer, c_q):
            (lat_a, rope_a), (lat_b, rope_b) = [q_heads(layer, c_q, uq[i], uk[i], cos_own, sin_own) for i in range(2)]
            return lat_a, lat_b, rope_a, rope_b

        normed = rms_norm(mine(x_in), attn_gain[0])
        c_q = rms_norm(jnp.dot(normed, w_dq[0], preferred_element_type=F32), q_gain[0])
        kv = jnp.dot(normed, w_dkv[0], preferred_element_type=F32)
        c_new0 = rms_norm(kv[:, :lat], kv_gain[0])
        k_new0 = rotate(kv[:, lat:], cos_own[:, :half], sin_own[:, half:rope]).astype(BF)
        k_pad0 = jnp.pad(k_new0, ((0, 0), (0, LANES - rope)))
        x_own, c_q, c_new1, k_pad1 = fused_layer(
            0, False, scale, pos_own, c_new0, k_pad0, uv, q_parts(0, c_q), ckv_2d, kpe_2d, x_in.reshape(CHUNKS, rows, width), mlp_gain[0:1], w_o2, w_gate, w_up, w_down,
            (attn_gain[1:2], q_gain[1:2], kv_gain[1:2], cos_t, sin_t, w_dq, w_dkv_t))
        c_new1 = c_new1.reshape(n, lat)
        k_pad1 = k_pad1.reshape(n, LANES)
        k_new1 = k_pad1[:, :rope]
        c_new0, k_new0 = whole(c_new0), whole(k_new0)
        x_out = fused_layer(1, True, scale, pos_own, mine(c_new1), mine(k_pad1), uv, q_parts(1, c_q.reshape(n // 2, -1)), ckv_2d, kpe_2d, x_own, mlp_gain[1:2], w_o2, w_gate, w_up, w_down, None)
        return x_out.reshape(n, width), jnp.stack([c_new0, c_new1]), jnp.stack([k_new0, k_new1])

    return jax.shard_map(device_body, mesh=mesh, in_specs=in_specs, out_specs=out_specs, check_vma=False)
```
